32 devices in a mesh: dp: 16 (over z, x, core), tensor: 2 (over y).
Axes of the slice: x: 2, y: 2, z: 4, core: 2. Of those that a mesh axis runs over, the one named last changes fastest.
Arguments:
- tokens: bfloat16 [32768, 768], P(('dp', 'tensor')), may hold values from -6 to 6
- seq_count: int32 [16], P('dp'), may hold values from 1 to 2, as said below
- first_gain: float32 [768], replicated, may hold values from 0.5 to 1.5
- first_shift: float32 [768], replicated, may hold values from -3 to 3
- heads_weight: bfloat16 [3, 768, 768], P(None, None, 'tensor'), may hold values from -0.21875 to 0.21875
- heads_bias: float32 [2, 768], P(None, 'tensor'), may hold values from -3 to 3
- mixing_weight: bfloat16 [768, 768], P('tensor'), may hold values from -1.75 to 1.75
- mixing_bias: float32 [768], replicated, may hold values from -3 to 3
- second_gain: float32 [768], replicated, may hold values from 0.5 to 1.5
- second_shift: float32 [768], replicated, may hold values from -3 to 3
- up_weight: bfloat16 [768, 3072], P(None, 'tensor'), may hold values from -0.21875 to 0.21875
- up_bias: float32 [3072], P('tensor'), may hold values from -3 to 3
- down_weight: bfloat16 [3072, 768], P('tensor'), may hold values from -0.3125 to 0.3125
- down_bias: float32 [768], replicated, may hold values from -3 to 3
- cotangent: bfloat16 [32768, 768], P(('dp', 'tensor')), may hold values from -6 to 6
Outputs:
- result: bfloat16 [32768, 768], P(('dp', 'tensor'))
- grad_tokens: bfloat16 [32768, 768], P(('dp', 'tensor'))
- grad_first_gain: float32 [768], replicated
- grad_first_shift: float32 [768], replicated
- grad_heads: float32 [3, 768, 768], P(None, None, 'tensor')
- grad_heads_bias: float32 [2, 768], P(None, 'tensor')
- grad_mixing: float32 [768, 768], P('tensor')
- grad_mixing_bias: float32 [768], replicated
- grad_second_gain: float32 [768], replicated
- grad_second_shift: float32 [768], replicated
- grad_up: float32 [768, 3072], P(None, 'tensor')
- grad_up_bias: float32 [3072], P('tensor')
- grad_down: float32 [3072, 768], P('tensor')
- grad_down_bias: float32 [768], replicated
The draws below stay inside these ranges and needn't reach their ends.
Inputs may be any that keep to these rules, and one draw needn't show every extreme that they name: Data group g holds seq_count[g] sequences of 2048 / seq_count[g] tokens each, one after the other; both values occur in every draw.
All inputs are finite; a program needn't handle non-finite values.
Results may differ from the reference program's by a relative error of at most 0.015.
Values may be sent and summed in bfloat16 or wider, within the bound.
A program may use at most 320 MiB of HBM per device.

```python
import math
import jax
import jax.numpy as jnp
from jax import lax

D = 768
FF = 3072
HEAD = 64
DEPTH = 12
TOK_DEV = 2048
TOKENS = 32768
N_DP = 16


def draw_seq_count(key, part):
    counts = jax.random.randint(key, (N_DP,), 1, 3, dtype=jnp.int32)
    return counts.at[0].set(1).at[1].set(2)


def steps_of(key, extent, split, least, largest):
    loudness, own = 1.0, jax.random.fold_in(key, 6)
    for dim, shards_of in split:
        steps = jnp.exp(jax.random.uniform(jax.random.fold_in(own, dim), (shards_of,), jnp.float32, least / len(split), largest / len(split)))
        loudness = loudness * jnp.repeat(steps, extent[dim] // shards_of).reshape([-1 if axis == dim else 1 for axis in range(len(extent))])
    return loudness


def normal_values(rng, dims, width, reach, shards=(), held_as=jnp.bfloat16):
    result = jax.random.normal(rng, dims, jnp.float32) * width
    if len(shards) > 0:
        result = steps_of(rng, dims, shards, -0.22, 0.18) * result
    return jnp.clip(result, min=-reach, max=reach).astype(held_as)


def setup_inputs(seed: int = 0) -> dict:
    seeds = jax.random.split(jax.random.key(seed), 16)
    return {
        "tokens": normal_values(seeds[0], (TOKENS, D), 1.0, 6.0, ((0, 32),)),
        "seq_count": draw_seq_count(jax.random.fold_in(seeds[15], 71), 0),
        "first_gain": jnp.clip(1.0 + 0.1 * jax.random.normal(seeds[2], (D,), jnp.float32), 0.5, 1.5),
        "first_shift": normal_values(seeds[3], (D,), 0.5, 3.0, (), jnp.float32),
        "heads_weight": normal_values(seeds[4], (3, D, D), D ** -0.5, 0.21875, ((2, 2),)),
        "heads_bias": normal_values(seeds[5], (2, D), 0.5, 3.0, ((1, 2),), jnp.float32),
        "mixing_weight": normal_values(seeds[6], (D, D), (D // 64) ** -0.5, 1.75, ((0, 2),)),
        "mixing_bias": normal_values(seeds[7], (D,), 0.5, 3.0, (), jnp.float32),
        "second_gain": jnp.clip(1.0 + 0.1 * jax.random.normal(seeds[8], (D,), jnp.float32), 0.5, 1.5),
        "second_shift": normal_values(seeds[9], (D,), 0.5, 3.0, (), jnp.float32),
        "up_weight": normal_values(seeds[10], (D, FF), D ** -0.5, 0.21875, ((1, 2),)),
        "up_bias": normal_values(seeds[11], (FF,), 0.5, 3.0, ((0, 2),), jnp.float32),
        "down_weight": normal_values(seeds[12], (FF, D), (FF // 8) ** -0.5, 0.3125, ((0, 2),)),
        "down_bias": normal_values(seeds[13], (D,), 0.5, 3.0, (), jnp.float32),
        "cotangent": normal_values(seeds[14], (TOKENS, D), 1.0, 6.0, ((0, 32),)),
    }


@jax.custom_vjp
def low(v):
    return lax.optimization_barrier(v.astype(jnp.bfloat16)).astype(jnp.float32)

@jax.custom_vjp
def low_back(v):
    return v

def low_keep(v):
    return (low(v), None)

def low_pass(kept, grad):
    return (grad,)

def back_keep(v):
    return (v, None)

def back_low(kept, grad):
    return (low(grad),)
low.defvjp(low_keep, low_pass)
low_back.defvjp(back_keep, back_low)
EPSILON = 1e-05
SCORE_SCALE = 0.125
HIGH = lax.Precision.HIGHEST

def normalize_rows(values, gain, shift):
    centre = lax.optimization_barrier(jnp.mean(values, axis=-1, keepdims=True))
    centred = values - centre
    spread = lax.optimization_barrier(jnp.mean(centred * centred, axis=-1, keepdims=True))
    return centred * lax.rsqrt(spread + EPSILON) * gain + shift

def gelu_tanh(values):
    return 0.5 * values * (1.0 + jnp.tanh(math.sqrt(2.0 / math.pi) * (values + 0.044715 * values * values * values)))

def seq_mask(first, count_rows, total, seq_total, key_rows):
    query_pos = first + lax.iota(jnp.int32, count_rows)
    key_pos = lax.iota(jnp.int32, key_rows)
    same = query_pos[:, None] * seq_total // total == key_pos[None, :] * seq_total // total
    return same & (key_pos[None, :] <= query_pos[:, None])

def block_forward(inputs, params, seq_total):
    first_gain, first_shift, heads_weight, heads_bias, mixing_weight, mixing_bias, second_gain, second_shift, up_weight, up_bias, down_weight, down_bias = params
    branch = 1.0 / math.sqrt(DEPTH)
    heads = D // HEAD
    normed_one = low(normalize_rows(inputs, first_gain, first_shift))
    bias_rows = jnp.stack([heads_bias[0], jnp.zeros_like(heads_bias[0]), heads_bias[1]])
    projected = jnp.einsum('rd,jde->jre', normed_one, heads_weight, precision=HIGH) + bias_rows[:, None, :]
    projected = low_back(low(projected))
    query = projected[0].reshape(TOK_DEV, heads, HEAD)
    keys = projected[1].reshape(TOK_DEV, heads, HEAD)
    values = projected[2].reshape(TOK_DEV, heads, HEAD)
    block_rows = min(512, TOK_DEV)

    def attend_block(index):
        start = index * block_rows
        query_block = lax.dynamic_slice_in_dim(query, start, block_rows, 0)
        scores = low_back(jnp.einsum('qhd,khd->hqk', query_block, keys, precision=HIGH) * SCORE_SCALE)
        allowed = seq_mask(start, block_rows, TOK_DEV, seq_total, TOK_DEV)
        scores = jnp.where(allowed[None], scores, -1e+30)
        peak = lax.optimization_barrier(jnp.max(scores, axis=-1, keepdims=True))
        expo = jnp.exp(scores - peak)
        probs = low(expo / lax.optimization_barrier(jnp.sum(expo, axis=-1, keepdims=True)))
        return jnp.einsum('hqk,khd->qhd', probs, values, precision=HIGH)
    attended = lax.map(jax.checkpoint(attend_block), jnp.arange(TOK_DEV // block_rows, dtype=jnp.int32))
    attended = low_back(low(attended.reshape(TOK_DEV, D)))
    mixed = low_back(jnp.dot(attended, mixing_weight, precision=HIGH))
    middle = inputs + branch * (mixed + mixing_bias)
    normed_two = low(normalize_rows(middle, second_gain, second_shift))
    pre_act = low_back(jnp.dot(normed_two, up_weight, precision=HIGH) + up_bias)
    activated = low(gelu_tanh(pre_act))
    down = low_back(jnp.dot(activated, down_weight, precision=HIGH))
    return middle + branch * (down + down_bias)

def reference(tokens, seq_count, first_gain, first_shift, heads_weight, heads_bias, mixing_weight, mixing_bias, second_gain, second_shift, up_weight, up_bias, down_weight, down_bias, cotangent):
    params = tuple((p.astype(jnp.float32) for p in (first_gain, first_shift, heads_weight, heads_bias, mixing_weight, mixing_bias, second_gain, second_shift, up_weight, up_bias, down_weight, down_bias)))
    groups = tokens.astype(jnp.float32).reshape(N_DP, TOK_DEV, D)
    cot_groups = cotangent.astype(jnp.float32).reshape(N_DP, TOK_DEV, D)

    def step(carry, item):
        rows_in, cot_in, seq_total = item
        output, pullback = jax.vjp(lambda inputs, weights: block_forward(inputs, weights, seq_total), rows_in, params)
        grad_in, grad_params = pullback(cot_in)
        carry = jax.tree.map(lambda left, right: left + right, carry, grad_params)
        return (carry, (output, grad_in))
    start_sums = jax.tree.map(jnp.zeros_like, params)
    sums, (outputs, grads_in) = lax.scan(step, start_sums, (groups, cot_groups, seq_count.astype(jnp.int32)))
    sums = tuple((s / N_DP for s in sums))
    return (outputs.reshape(TOKENS, D).astype(jnp.bfloat16), grads_in.reshape(TOKENS, D).astype(jnp.bfloat16), sums[0], sums[1], sums[2], sums[3], sums[4], sums[5], sums[6], sums[7], sums[8], sums[9], sums[10], sums[11])
```

```python
import functools, math
import jax
import jax.numpy as jnp
from jax import lax
from jax.experimental import pallas as pl
from jax.experimental.pallas import tpu as pltpu
from jax.sharding import PartitionSpec as P

HEAD = 64
LOG2E = math.log2(math.e)
NT = (((1,), (1,)), ((), ()))
TN = (((0,), (0,)), ((), ()))
f32 = jnp.float32
bf16 = jnp.bfloat16


def attn_forward_kernel(blk, info, own_ref, oth_ref, w_ref, b_ref, qkv_ref, att_ref, lse_ref, acc_ref, top_ref):
    qb = pl.program_id(0)
    nb = pl.num_programs(0)
    half = own_ref.shape[0]
    width = w_ref.shape[2]
    side, count = info[0], info[1]

    @pl.when(qb == 0)
    def _():
        step = 256
        for part, ref in enumerate((own_ref, oth_ref)):
            def rows_loop(i, _, part=part, ref=ref):
                rows = ref[pl.ds(pl.multiple_of(i * step, step), step), :]
                to = pl.multiple_of(part * half + i * step, step)
                for j in range(3):
                    y = jnp.dot(rows, w_ref[j], preferred_element_type=f32) + b_ref[pl.ds(j, 1), :]
                    y = y.astype(bf16)
                    if j == 0:
                        y = y * bf16(0.125)
                    qkv_ref[j, pl.ds(to, step), :] = y
                return 0
            lax.fori_loop(0, half // step, rows_loop, 0)

    def place(b):
        return pl.multiple_of(lax.rem(b + side * (nb // 2), nb) * blk, blk)

    lane_lo = lax.broadcasted_iota(jnp.int32, (blk, 128), 1) < HEAD
    first = (qb * count // nb) * nb // count
    q_at = place(qb)

    def block(kb, fresh, masked):
        k_at = place(kb)
        if masked:
            qi = lax.broadcasted_iota(jnp.int32, (blk, blk), 0)
            ki = lax.broadcasted_iota(jnp.int32, (blk, blk), 1)
            keep = ki <= qi
        for p in range(width // 128):
            cols = pl.ds(128 * p, 128)
            q = qkv_ref[0, pl.ds(q_at, blk), cols]
            k = qkv_ref[1, pl.ds(k_at, blk), cols]
            v = qkv_ref[2, pl.ds(k_at, blk), cols]
            for h in range(2):
                mine = lane_lo if h == 0 else ~lane_lo
                head = 2 * p + h
                qh = jnp.where(mine, q, bf16(0))
                vh = jnp.where(mine, v, bf16(1))
                s = lax.dot_general(qh, k, NT, preferred_element_type=f32) * LOG2E
                if masked:
                    s = jnp.where(keep, s, -1e30)
                top = jnp.max(s, axis=1, keepdims=True)
                if fresh:
                    e = jnp.exp2(s - top)
                    acc_ref[head] = jnp.dot(e.astype(bf16), vh, preferred_element_type=f32)
                    top_ref[head] = jnp.broadcast_to(top, (blk, 128))
                else:
                    old = top_ref[head]
                    new = jnp.maximum(old, top)
                    e = jnp.exp2(s - new[:, :1])
                    acc_ref[head] = acc_ref[head] * jnp.exp2(old - new) + jnp.dot(
                        e.astype(bf16), vh, preferred_element_type=f32)
                    top_ref[head] = new

    block(qb, True, True)

    def loop(kb, _):
        block(kb, False, False)
        return 0
    lax.fori_loop(first, qb, loop, 0)

    for p in range(width // 128):
        a0, a1 = acc_ref[2 * p], acc_ref[2 * p + 1]
        num = jnp.where(lane_lo, a0, a1)
        den = jnp.where(lane_lo, pltpu.roll(a0, HEAD, 1), pltpu.roll(a1, HEAD, 1))
        att_ref[pl.ds(q_at, blk), pl.ds(128 * p, 128)] = (num / den).astype(bf16)
        logs = jnp.where(lane_lo, top_ref[2 * p], top_ref[2 * p + 1]) + jnp.log2(den)
        rows = logs.T
        lse_ref[qb, pl.ds(2 * p, 1), :] = rows[0:1]
        lse_ref[qb, pl.ds(2 * p + 1, 1), :] = rows[HEAD:HEAD + 1]


def attn_forward(info, own, oth, w, b, blk=512):
    half = own.shape[0]
    rows = 2 * half
    width = w.shape[2]
    nb = rows // blk
    heads = width // HEAD
    vm = pl.BlockSpec(memory_space=pltpu.VMEM)
    return pl.pallas_call(
        functools.partial(attn_forward_kernel, blk),
        grid=(nb,),
        in_specs=[pl.BlockSpec(memory_space=pltpu.SMEM), vm, vm, vm, vm],
        out_specs=[vm, vm, vm],
        out_shape=[jax.ShapeDtypeStruct((3, rows, width), bf16),
                   jax.ShapeDtypeStruct((rows, width), bf16),
                   jax.ShapeDtypeStruct((nb, 8, blk), f32)],
        scratch_shapes=[pltpu.VMEM((heads, blk, 128), f32), pltpu.VMEM((heads, blk, 128), f32)],
        compiler_params=pltpu.CompilerParams(vmem_limit_bytes=56 << 20),
        cost_estimate=pl.CostEstimate(flops=12_000_000_000, transcendentals=0, bytes_accessed=12_000_000),
        name="attn_forward",
    )(info, own, oth, w, b)


def attn_backward_kernel(blk, info, qkv_ref, att_ref, gown_ref, goth_ref, lse_ref, out_ref, g_ref, delta_ref, dq_ref, dk_ref, dv_ref):
    kb = pl.program_id(0)
    nb = pl.num_programs(0)
    half = gown_ref.shape[0]
    width = gown_ref.shape[1]
    heads = width // HEAD
    side, count = info[0], info[1]

    def place(b):
        return pl.multiple_of(lax.rem(b + side * (nb // 2), nb) * blk, blk)

    @pl.when(kb == 0)
    def _():
        g_ref[pl.ds(0, half), :] = gown_ref[...]
        g_ref[pl.ds(half, half), :] = goth_ref[...]
        dq_ref[...] = jnp.zeros_like(dq_ref)
        pick = (lax.broadcasted_iota(jnp.int32, (8, width), 1) // HEAD
                == lax.broadcasted_iota(jnp.int32, (8, width), 0)).astype(bf16)

        def deltas(b, _):
            at = place(b)
            prod = g_ref[pl.ds(at, blk), :].astype(f32) * att_ref[pl.ds(at, blk), :].astype(f32)
            high = prod.astype(bf16)
            low = (prod - high.astype(f32)).astype(bf16)
            delta_ref[b] = (lax.dot_general(pick, high, NT, preferred_element_type=f32)
                            + lax.dot_general(pick, low, NT, preferred_element_type=f32))
            return 0
        lax.fori_loop(0, nb, deltas, 0)

    lane_lo = lax.broadcasted_iota(jnp.int32, (blk, 128), 1) < HEAD
    k_at = place(kb)

    def block(qb, masked):
        q_at = place(qb)
        if masked:
            ki = lax.broadcasted_iota(jnp.int32, (blk, blk), 0)
            qi = lax.broadcasted_iota(jnp.int32, (blk, blk), 1)
            keep = ki <= qi
        for p in range(width // 128):
            cols = pl.ds(128 * p, 128)
            q = qkv_ref[0, pl.ds(q_at, blk), cols]
            g = g_ref[pl.ds(q_at, blk), cols]
            k = qkv_ref[1, pl.ds(k_at, blk), cols]
            v = qkv_ref[2, pl.ds(k_at, blk), cols]
            dk = dv = dq = None
            for h in range(2):
                mine = lane_lo if h == 0 else ~lane_lo
                head = 2 * p + h
                kh = jnp.where(mine, k, bf16(0))
                vh = jnp.where(mine, v, bf16(0))
                s = lax.dot_general(kh, q, NT, preferred_element_type=f32) * LOG2E
                e = jnp.exp2(s - lse_ref[qb, pl.ds(head, 1), :])
                if masked:
                    e = jnp.where(keep, e, 0.0)
                dp = lax.dot_general(vh, g, NT, preferred_element_type=f32)
                ds = (e * (dp - delta_ref[qb, pl.ds(head, 1), :])).astype(bf16)
                e = e.astype(bf16)
                dv1 = jnp.dot(e, jnp.where(mine, g, bf16(0)), preferred_element_type=f32)
                dk1 = jnp.dot(ds, jnp.where(mine, q, bf16(0)), preferred_element_type=f32)
                dq1 = lax.dot_general(ds, kh, TN, preferred_element_type=f32)
                dk, dv, dq = (dk1, dv1, dq1) if h == 0 else (dk + dk1, dv + dv1, dq + dq1)
            if masked:
                dk_ref[:, cols] = dk
                dv_ref[:, cols] = dv
            else:
                dk_ref[:, cols] += dk
                dv_ref[:, cols] += dv
            dq_ref[pl.ds(q_at, blk), cols] += dq

    block(kb, True)
    last = ((kb * count // nb) + 1) * nb // count

    def loop(qb, _):
        block(qb, False)
        return 0
    lax.fori_loop(kb + 1, last, loop, 0)
    out_ref[1, pl.ds(k_at, blk), :] = dk_ref[...].astype(bf16)
    out_ref[2, pl.ds(k_at, blk), :] = dv_ref[...].astype(bf16)

    out_ref[0, pl.ds(k_at, blk), :] = (dq_ref[pl.ds(k_at, blk), :] * 0.125).astype(bf16)


def attn_backward(info, qkv, att, gown, goth, lse, blk=512):
    rows, width = att.shape
    nb = rows // blk
    vm = pl.BlockSpec(memory_space=pltpu.VMEM)
    return pl.pallas_call(
        functools.partial(attn_backward_kernel, blk),
        grid=(nb,),
        in_specs=[pl.BlockSpec(memory_space=pltpu.SMEM)] + [vm] * 5,
        out_specs=vm,
        out_shape=jax.ShapeDtypeStruct((3, rows, width), bf16),
        scratch_shapes=[pltpu.VMEM((rows, width), bf16), pltpu.VMEM((nb, 8, blk), f32),
                        pltpu.VMEM((rows, width), f32), pltpu.VMEM((blk, width), f32),
                        pltpu.VMEM((blk, width), f32)],
        compiler_params=pltpu.CompilerParams(vmem_limit_bytes=56 << 20),
        cost_estimate=pl.CostEstimate(flops=30_000_000_000, transcendentals=0, bytes_accessed=14_000_000),
        name="attn_backward",
    )(info, qkv, att, gown, goth, lse)


DEPTH = 12
EPSILON = 1e-05
BRANCH = 1.0 / math.sqrt(DEPTH)
GELU_C = math.sqrt(2.0 / math.pi)
SWAP = ((0, 1), (1, 0))


def to_peer(v):
    return lax.ppermute(v, "tensor", SWAP)


def row_stats(v):
    centre = jnp.mean(v, axis=-1, keepdims=True)
    centred = v - centre
    inv = lax.rsqrt(jnp.mean(centred * centred, axis=-1, keepdims=True) + EPSILON)
    return centre, inv


def norm_back(e, gain, h, inv):
    eg = e * gain
    return inv * (eg - jnp.mean(eg, axis=-1, keepdims=True)
                  - h * jnp.mean(eg * h, axis=-1, keepdims=True))


def add16(a, b):
    return (a.astype(f32) + b.astype(f32)).astype(bf16)


def dot32(a, b):
    return jnp.dot(a, b, preferred_element_type=f32)


def dot_nt(a, b):
    return lax.dot_general(a, b, NT, preferred_element_type=f32)


def dot_tn(a, b):
    return lax.dot_general(a, b, TN, preferred_element_type=f32)


def xor_step(v, size, bit):
    return lax.ppermute(v, "dp", [(i, i ^ (1 << bit)) for i in range(size)])


def sum_small(v, size):
    for bit in range(size.bit_length() - 1):
        v = v + xor_step(v, size, bit)
    return v


def halving_sum(v, size, me):
    bits = size.bit_length() - 1
    for bit in range(bits):
        half = v.shape[0] // 2
        side = (me >> bit) & 1
        keep = lax.dynamic_slice_in_dim(v, side * half, half, 0)
        send = lax.dynamic_slice_in_dim(v, (1 - side) * half, half, 0)
        v = add16(keep, xor_step(send, size, bit))
    for bit in reversed(range(bits)):
        side = (me >> bit) & 1
        other = xor_step(v, size, bit)
        v = jnp.where(side == 0, jnp.concatenate([v, other]), jnp.concatenate([other, v]))
    return v


def ring_plan(size):
    chips = size // 2
    order = list(range(0, chips, 2)) + list(range(1, chips, 2))[::-1]
    table = [0] * size
    pairs = []
    for p, chip in enumerate(order):
        table[2 * chip] = p
        table[2 * chip + 1] = (chips - p) % chips
        pairs.append((2 * chip, 2 * order[(p + 1) % chips]))
        pairs.append((2 * chip + 1, 2 * order[(p - 1) % chips] + 1))
    return chips, table, pairs


def ring_reduce(first, second, size, me):
    chips, table, pairs = ring_plan(size)
    core = me % 2
    send = jnp.where(core == 0, second, first)
    keep = jnp.where(core == 0, first, second)
    mate = xor_step(send, size, 0)
    rows, width = first.shape[1:]
    ch = rows // chips
    keep = add16(keep, mate).reshape(2, chips, ch, width)
    pos = jnp.array(table, jnp.int32)[me]

    def chunk(i):
        return lax.dynamic_index_in_dim(keep, lax.rem(i + 2 * chips, chips), 1, keepdims=False)

    moving = chunk(pos)
    for s in range(chips - 1):
        moving = add16(lax.ppermute(moving, "dp", pairs), chunk(pos - s - 1))
    done = add16(moving[0], to_peer(moving[1]))
    full = jnp.zeros((chips, ch, width), bf16)
    full = lax.dynamic_update_index_in_dim(full, done, lax.rem(pos + 1, chips), 0)
    for s in range(chips - 1):
        done = lax.ppermute(done, "dp", pairs)
        full = lax.dynamic_update_index_in_dim(full, done, lax.rem(pos - s + chips, chips), 0)
    full = full.reshape(rows, width)
    other = xor_step(full, size, 0)
    return jnp.where(core == 0, full, other), jnp.where(core == 0, other, full)


def gelu_pair(v):
    t = jnp.tanh(GELU_C * (v + 0.044715 * v * v * v))
    return 0.5 * v * (1.0 + t), 0.5 * (1.0 + t) + 0.5 * v * (1.0 - t * t) * (
        GELU_C * (1.0 + 3.0 * 0.044715 * v * v))


def local(
    tokens,
    seq_count,
    first_gain,
    first_shift,
    heads_weight,
    heads_bias,
    mixing_weight,
    mixing_bias,
    second_gain,
    second_shift,
    up_weight,
    up_bias,
    down_weight,
    down_bias,
    cotangent,
):
    size = lax.axis_size("dp")
    me = lax.axis_index("dp")
    side = lax.axis_index("tensor")
    info = jnp.stack([side.astype(jnp.int32), seq_count[0]])
    half, dim = tokens.shape
    width = heads_weight.shape[2]
    hidden = up_weight.shape[1]

    pu, pd, pm = dim // size, hidden // size, width // size
    piece = jnp.concatenate([
        lax.dynamic_slice(up_weight, (me * pu, 0), (pu, hidden // 2)),
        lax.dynamic_slice(up_weight, (me * pu, hidden // 2), (pu, hidden // 2)),
        lax.dynamic_slice_in_dim(down_weight, me * pd, pd, 0),
        lax.dynamic_slice_in_dim(mixing_weight, me * pm, pm, 0)])
    packed = lax.all_gather(to_peer(piece), "dp", axis=0)
    up_other = jnp.concatenate([packed[:, :pu].reshape(dim, hidden // 2),
                                packed[:, pu:2 * pu].reshape(dim, hidden // 2)], axis=1)
    down_other = packed[:, 2 * pu:2 * pu + pd].reshape(hidden, dim)
    mix_other = packed[:, 2 * pu + pd:].reshape(width, dim)
    up_bias_other = to_peer(up_bias)

    x = tokens.astype(f32)
    centre1, inv1 = row_stats(x)
    a1 = ((x - centre1) * inv1 * first_gain + first_shift).astype(bf16)
    a1_other = to_peer(a1)
    bias3 = jnp.stack([heads_bias[0], jnp.zeros_like(heads_bias[0]), heads_bias[1]])
    qkv, att, lse = attn_forward(info, a1, a1_other, heads_weight, bias3)
    att_mine = att[:half]
    att_recv = to_peer(att[half:])
    middle = x + BRANCH * (dot32(att_mine, mixing_weight) + dot32(att_recv, mix_other) + mixing_bias)
    centre2, inv2 = row_stats(middle)
    h2 = (middle - centre2) * inv2
    a2 = (h2 * second_gain + second_shift).astype(bf16)

    g_out = cotangent.astype(f32)
    grad_mlp = (BRANCH * g_out).astype(bf16)
    down_sum = 0.0
    grad_a2 = 0.0
    grads_up, grads_down, bias_up = [], [], []
    for up, bias, down in ((up_weight, up_bias, down_weight), (up_other, up_bias_other, down_other)):
        pre = dot32(a2, up) + bias
        act, slope = gelu_pair(pre)
        act = act.astype(bf16)
        down_sum += dot32(act, down)
        grad_pre = (dot_nt(grad_mlp, down) * slope).astype(bf16)
        grads_down.append(dot_tn(act, grad_mlp).astype(bf16))
        grads_up.append(jnp.concatenate([dot_tn(a2, grad_pre[:, :hidden // 2]),
                                         dot_tn(a2, grad_pre[:, hidden // 2:])]).astype(bf16))
        bias_up.append(jnp.sum(grad_pre, axis=0, dtype=f32).reshape(2, dim))
        grad_a2 += dot_nt(grad_pre, up)
    result = (middle + BRANCH * (down_sum + down_bias)).astype(bf16)
    grad_down, grad_up = ring_reduce(jnp.stack(grads_down), jnp.stack(grads_up), size, me)

    grad_middle = g_out + norm_back(grad_a2, second_gain, h2, inv2)
    grad_attn = (BRANCH * grad_middle).astype(bf16)
    g_own = dot_nt(grad_attn, mixing_weight).astype(bf16)
    g_other = to_peer(dot_nt(grad_attn, mix_other).astype(bf16))
    small = jnp.concatenate([
        jnp.stack([BRANCH * jnp.sum(g_out, axis=0), jnp.sum(grad_a2 * h2, axis=0),
                   jnp.sum(grad_a2, axis=0), BRANCH * jnp.sum(grad_middle, axis=0)])] + bias_up)
    small = sum_small(small, size)
    small = small[:6] + to_peer(jnp.concatenate([small[:4], small[6:8]]))
    grad_mix = add16(dot_tn(att_mine, grad_attn), to_peer(dot_tn(att_recv, grad_attn).astype(bf16)))

    gqkv = attn_backward(info, qkv, att, g_own, g_other, lse)
    gq_mine, gq_other = gqkv[:, :half], gqkv[:, half:]

    def back_heads(gq):
        return sum(dot_nt(gq[j], heads_weight[j]) for j in range(3))

    sent = to_peer(back_heads(gq_other).astype(bf16))
    grad_a1 = back_heads(gq_mine) + sent.astype(f32)
    grad_heads = [(dot_tn(a1, gq_mine[j]) + dot_tn(a1_other, gq_other[j])).astype(bf16) for j in range(3)]
    tail = jnp.concatenate(grad_heads + [grad_mix[:, :width], grad_mix[:, width:]])
    tail = halving_sum(tail, size, me)

    h1 = (x - centre1) * inv1
    grad_tokens = (grad_middle + norm_back(grad_a1, first_gain, h1, inv1)).astype(bf16)
    grad_hb = jnp.concatenate([jnp.sum(gqkv[0], axis=0, dtype=f32), jnp.sum(gqkv[2], axis=0, dtype=f32)])
    last = jnp.stack([jnp.sum(grad_a1 * h1, axis=0), jnp.sum(grad_a1, axis=0), grad_hb])
    last = sum_small(last, size)
    first_two = last[:2] + to_peer(last[:2])
    groups = 1.0 / size
    first_two = first_two * groups
    small = small * groups
    tail = tail.astype(f32) * groups
    grad_up = grad_up.astype(f32) * groups
    return (
        result,
        grad_tokens,
        first_two[0],
        first_two[1],
        tail[:3 * dim].reshape(3, dim, width),
        last[2].reshape(2, width) * groups,
        jnp.concatenate([tail[3 * dim:3 * dim + width], tail[3 * dim + width:]], axis=1),
        small[3],
        small[1],
        small[2],
        jnp.concatenate([grad_up[:dim], grad_up[dim:]], axis=1),
        small[4:6].reshape(hidden),
        grad_down.astype(f32) * groups,
        small[0],
    )


def solution(mesh):
    placed = (
        P(("dp", "tensor"), None),
        P("dp"),
        P(),
        P(),
        P(None, None, "tensor"),
        P(None, "tensor"),
        P("tensor", None),
        P(),
        P(),
        P(),
        P(None, "tensor"),
        P("tensor"),
        P("tensor", None),
        P(),
        P(("dp", "tensor"), None),
    )
    return jax.shard_map(
        local,
        mesh=mesh,
        in_specs=placed,
        out_specs=(
            P(("dp", "tensor"), None),
            P(("dp", "tensor"), None),
            P(),
            P(),
            P(None, None, "tensor"),
            P(None, "tensor"),
            P("tensor", None),
            P(),
            P(),
            P(),
            P(None, "tensor"),
            P("tensor"),
            P("tensor", None),
            P(),
        ),
        check_vma=False,
    )
```

```python
import functools, math
import jax
import jax.numpy as jnp
from jax import lax
from jax.experimental import pallas as pl
from jax.experimental.pallas import tpu as pltpu
from jax.sharding import PartitionSpec as P

HEAD = 64
DEPTH = 12
EPSILON = 1e-05
BRANCH = 1.0 / math.sqrt(DEPTH)
GELU_C = math.sqrt(2.0 / math.pi)
SWAP = ((0, 1), (1, 0))
LOG2E = math.log2(math.e)
NT = (((1,), (1,)), ((), ()))
TN = (((0,), (0,)), ((), ()))
f32 = jnp.float32
bf16 = jnp.bfloat16


def attn_forward_kernel(blk, info, own_ref, oth_ref, w_ref, b_ref, qkv_ref, att_ref, lse_ref, acc_ref, top_ref):
    qb = pl.program_id(0)
    nb = pl.num_programs(0)
    half = own_ref.shape[0]
    width = w_ref.shape[2]
    side, count = info[0], info[1]

    @pl.when(qb == 0)
    def _():
        step = 256
        for part, ref in enumerate((own_ref, oth_ref)):
            def rows_loop(i, _, part=part, ref=ref):
                rows = ref[pl.ds(pl.multiple_of(i * step, step), step), :]
                to = pl.multiple_of(part * half + i * step, step)
                for j in range(3):
                    y = jnp.dot(rows, w_ref[j], preferred_element_type=f32) + b_ref[pl.ds(j, 1), :]
                    y = y.astype(bf16)
                    if j == 0:
                        y = y * bf16(0.125)
                    qkv_ref[pl.ds(to, step), pl.ds(j * width, width)] = y
                return 0
            lax.fori_loop(0, half // step, rows_loop, 0)

    def place(b):
        return pl.multiple_of(lax.rem(b + side * (nb // 2), nb) * blk, blk)

    lane_lo = lax.broadcasted_iota(jnp.int32, (blk, 128), 1) < HEAD
    first = (qb * count // nb) * nb // count
    q_at = place(qb)

    def block(kb, fresh, masked):
        k_at = place(kb)
        if masked:
            qi = lax.broadcasted_iota(jnp.int32, (blk, blk), 0)
            ki = lax.broadcasted_iota(jnp.int32, (blk, blk), 1)
            keep = ki <= qi
        for p in range(width // 128):
            q = qkv_ref[pl.ds(q_at, blk), pl.ds(0 * width + 128 * p, 128)]
            k = qkv_ref[pl.ds(k_at, blk), pl.ds(1 * width + 128 * p, 128)]
            v = qkv_ref[pl.ds(k_at, blk), pl.ds(2 * width + 128 * p, 128)]
            for h in range(2):
                mine = lane_lo if h == 0 else ~lane_lo
                head = 2 * p + h
                qh = jnp.where(mine, q, bf16(0))
                vh = jnp.where(mine, v, bf16(1))
                s = lax.dot_general(qh, k, NT, preferred_element_type=f32) * LOG2E
                if masked:
                    s = jnp.where(keep, s, -1e30)
                top = jnp.max(s, axis=1, keepdims=True)
                if fresh:
                    e = jnp.exp2(s - top)
                    acc_ref[head] = jnp.dot(e.astype(bf16), vh, preferred_element_type=f32)
                    top_ref[head] = jnp.broadcast_to(top, (blk, 128))
                else:
                    old = top_ref[head]
                    new = jnp.maximum(old, top)
                    e = jnp.exp2(s - new[:, :1])
                    acc_ref[head] = acc_ref[head] * jnp.exp2(old - new) + jnp.dot(
                        e.astype(bf16), vh, preferred_element_type=f32)
                    top_ref[head] = new

    block(qb, True, True)

    def loop(kb, _):
        block(kb, False, False)
        return 0
    lax.fori_loop(first, qb, loop, 0)

    for p in range(width // 128):
        a0, a1 = acc_ref[2 * p], acc_ref[2 * p + 1]
        num = jnp.where(lane_lo, a0, a1)
        den = jnp.where(lane_lo, pltpu.roll(a0, HEAD, 1), pltpu.roll(a1, HEAD, 1))
        att_ref[pl.ds(q_at, blk), pl.ds(128 * p, 128)] = (num / den).astype(bf16)
        logs = jnp.where(lane_lo, top_ref[2 * p], top_ref[2 * p + 1]) + jnp.log2(den)
        rows = logs.T
        lse_ref[qb, pl.ds(2 * p, 1), :] = rows[0:1]
        lse_ref[qb, pl.ds(2 * p + 1, 1), :] = rows[HEAD:HEAD + 1]


def attn_forward(info, own, oth, w, b, blk=512):
    half = own.shape[0]
    rows = 2 * half
    width = w.shape[2]
    nb = rows // blk
    heads = width // HEAD
    vm = pl.BlockSpec(memory_space=pltpu.VMEM)
    return pl.pallas_call(
        functools.partial(attn_forward_kernel, blk),
        grid=(nb,),
        in_specs=[pl.BlockSpec(memory_space=pltpu.SMEM), vm, vm, vm, vm],
        out_specs=[vm, vm, vm],
        out_shape=[jax.ShapeDtypeStruct((rows, 3 * width), bf16),
                   jax.ShapeDtypeStruct((rows, width), bf16),
                   jax.ShapeDtypeStruct((nb, 8, blk), f32)],
        scratch_shapes=[pltpu.VMEM((heads, blk, 128), f32), pltpu.VMEM((heads, blk, 128), f32)],
        compiler_params=pltpu.CompilerParams(vmem_limit_bytes=56 << 20),
        cost_estimate=pl.CostEstimate(flops=12_000_000_000, transcendentals=0, bytes_accessed=12_000_000),
        name="attn_forward",
    )(info, own, oth, w, b)


def ring_reduce_ticks(n, parts, local, refs, spot, dest):
    mate, slot, first, yin, fin, s_send, s_recv, a_send, a_recv, m_send, m_recv, y_sem = refs
    core, pos = spot["core"], spot["pos"]

    def put(src, dst, send, recv, to):
        return pltpu.make_async_remote_copy(src_ref=src, dst_ref=dst, send_sem=send, recv_sem=recv,
                                            device_id=dest[to], device_id_type=pl.DeviceIdType.MESH)

    def at(c):
        return lax.rem(c + 2 * n, n)

    def ring_copy(s):
        src = slot.at[jnp.maximum(s - 1, 0)]
        return put(src, slot.at[s], s_send.at[s], s_recv.at[s], "next")

    def gather_copy(s):
        c = core * n + at(pos + 1 - s)
        return put(fin.at[c], fin.at[c], a_send.at[s], a_recv.at[s], "next")

    def arrived(s):
        c = core * n + at(pos - s)
        return put(fin.at[c], fin.at[c], a_send.at[s], a_recv.at[s], "next")

    def mate_copy(s):
        c = core * n + at(pos + 1 - s)
        return put(fin.at[c], fin.at[c], m_send.at[s], m_recv.at[s], "mate")

    def mate_arrived(s):
        return put(fin.at[0], fin.at[0], m_send.at[s], m_recv.at[s], "mate")

    first_copy = put(first, slot.at[0], s_send.at[0], s_recv.at[0], "next")
    if parts == 2:
        y_copy = put(slot.at[n - 2, 1], yin, y_sem.at[0], y_sem.at[1], "peer")

    def tick(k):
        @pl.when(k == 0)
        def _():
            for part in range(parts):
                first[part] = (local(part, at(pos)).astype(f32) + mate[part, at(pos)].astype(f32)).astype(bf16)
            first_copy.start()

        @pl.when((k > 0) & (k < n))
        def _():
            s = k - 1
            put(slot.at[s], slot.at[s], s_send.at[s], s_recv.at[s], "next").wait_recv()
            c = at(pos - k)
            for part in range(parts):
                slot[s, part] = (slot[s, part].astype(f32) + local(part, c).astype(f32)
                                 + mate[part, c].astype(f32)).astype(bf16)

            @pl.when(k < n - 1)
            def _():
                ring_copy(k).start()
            if parts == 2:
                @pl.when(k == n - 1)
                def _():
                    y_copy.start()

        @pl.when(k == n)
        def _():
            if parts == 2:
                y_copy.wait_recv()
                fin[core * n + at(pos + 1)] = (slot[n - 2, 0].astype(f32) + yin[...].astype(f32)).astype(bf16)
            else:
                fin[core * n + at(pos + 1)] = slot[n - 2, 0]
            gather_copy(0).start()
            mate_copy(0).start()

        @pl.when(k > n)
        def _():
            s = k - n - 1
            arrived(s).wait_recv()

            @pl.when(s < n - 2)
            def _():
                gather_copy(s + 1).start()
            mate_copy(s + 1).start()

    def finish():
        first_copy.wait_send()

        def sends(s, _):
            ring_copy(s).wait_send()
            return 0
        lax.fori_loop(1, n - 1, sends, 0)
        if parts == 2:
            y_copy.wait_send()

        def gathers(s, _):
            gather_copy(s).wait_send()
            return 0
        lax.fori_loop(0, n - 1, gathers, 0)

        def mates(s, _):
            mate_copy(s).wait_send()
            mate_arrived(s).wait_recv()
            return 0
        lax.fori_loop(0, n, mates, 0)

    return tick, finish


def backward_kernel(size, blk, count_ref, qkv_hbm, att_ref, gown_hbm, goth_hbm, lse_ref, gw_hbm, own_ref, oth_ref,
                    w_hbm, gmix_hbm, small_ref, tok_ref, gain_ref, gm_ref,
                    fin_ref, tail_ref, gtok_ref, small_out, last_out,
                    qkv_ref, g_ref, delta_ref, dq_ref, dk_ref, dv_ref, w_ref,
                    gl_ref, mate_ref, slot_ref, first_ref, yin_ref,
                    t_ref, tmate_ref, tslot_ref, tfirst_ref,
                    da_ref, dsend_ref, drecv_ref, vb_ref, rb_ref, ub_ref, qb_ref, hb_ref,
                    in_sem, c_sem, s_send, s_recv, a_send, a_recv, m_send, m_recv, y_sem,
                    tc_sem, ts_send, ts_recv, ta_send, ta_recv, tm_send, tm_recv,
                    d_send, d_recv, v_send, v_recv, u_send, u_recv):
    n = size // 2
    bits = size.bit_length() - 1
    rows, total = qkv_ref.shape
    half = rows // 2
    width = total // 3
    dim = own_ref.shape[1]
    nb = rows // blk
    me, side = lax.axis_index("dp"), lax.axis_index("tensor")
    core, chip = lax.rem(me, 2), me // 2
    odd = lax.rem(chip, 2)
    p = (1 - odd) * (chip // 2) + odd * (n - 1 - chip // 2)

    def chip_at(q):
        up = q // (n // 2)
        return (1 - up) * 2 * q + up * (2 * (n - 1 - q) + 1)
    pos = (1 - core) * p + core * lax.rem(n - p, n)
    step = 1 - 2 * core
    dest = {
        "next": {"dp": 2 * chip_at(lax.rem(p + step + n, n)) + core},
        "prev": {"dp": 2 * chip_at(lax.rem(p - step + n, n)) + core},
        "mate": {"dp": me + 1 - 2 * core},
        "peer": {"tensor": 1 - side},
    }
    for b in range(1, bits):
        dest[b] = {"dp": me + (1 - 2 * lax.rem(me // (1 << b), 2)) * (1 << b)}
    dest[0] = dest["mate"]
    dest[bits] = dest["peer"]

    def fetch(src, dst, i):
        copy = pltpu.make_async_copy(src, dst, in_sem.at[i])
        copy.start()
        return copy
    gl_copy = fetch(gw_hbm.at[core], gl_ref, 0)
    q_copy = fetch(qkv_hbm, qkv_ref, 1)
    g0_copy = fetch(gown_hbm, g_ref.at[pl.ds(0, half)], 2)
    g1_copy = fetch(goth_hbm, g_ref.at[pl.ds(half, half)], 3)
    w_copies = [fetch(w_hbm.at[j], w_ref.at[:, pl.ds(j * width, width)], 4 + j) for j in range(3)]
    ch2 = t_ref.shape[1]
    gx_copy = fetch(gmix_hbm, t_ref.at[pl.ds(3 * dim // ch2, dim // ch2)], 7)

    barrier = pltpu.get_barrier_semaphore()
    friends = ["next", "prev", "mate", "peer"] + list(range(1, bits))
    for to in friends:
        pl.semaphore_signal(barrier, inc=1, device_id=dest[to], device_id_type=pl.DeviceIdType.MESH)
    pl.semaphore_wait(barrier, len(friends))

    def put(src, dst, send, recv, to):
        return pltpu.make_async_remote_copy(src_ref=src, dst_ref=dst, send_sem=send, recv_sem=recv,
                                            device_id=dest[to], device_id_type=pl.DeviceIdType.MESH)
    core_copy = put(gw_hbm.at[1 - core], mate_ref, c_sem.at[0], c_sem.at[1], "mate")
    core_copy.start()
    vb_ref[0] = small_ref[...]

    spot = {"core": core, "pos": pos}
    tick, finish = ring_reduce_ticks(
        n, 2, lambda part, c: gl_ref[part, c],
        (mate_ref, slot_ref, first_ref, yin_ref, fin_ref, s_send, s_recv, a_send, a_recv, m_send, m_recv, y_sem),
        spot, dest)
    ttick, tfinish = ring_reduce_ticks(
        n, 1, lambda part, c: t_ref[core * n + c],
        (tmate_ref, tslot_ref, tfirst_ref, None, tail_ref, ts_send, ts_recv, ta_send, ta_recv, tm_send, tm_recv,
         y_sem),
        spot, dest)

    def small_copy(buf, inbox, send, recv, b):
        return put(buf.at[b], inbox.at[b], send.at[b], recv.at[b], b)

    def small_start(b):
        small_copy(vb_ref, rb_ref, v_send, v_recv, b).start()

    def small_end(b):
        small_copy(vb_ref, rb_ref, v_send, v_recv, b).wait()
        if b < bits:
            vb_ref[b + 1] = vb_ref[b] + rb_ref[b]

    small_start(0)
    q_copy.wait()
    g0_copy.wait()
    g1_copy.wait()
    dq_ref[...] = jnp.zeros_like(dq_ref)
    hb_ref[...] = jnp.zeros_like(hb_ref)

    def place(b):
        return pl.multiple_of(lax.rem(b + side * (nb // 2), nb) * blk, blk)
    pick = (lax.broadcasted_iota(jnp.int32, (8, width), 1) // HEAD
            == lax.broadcasted_iota(jnp.int32, (8, width), 0)).astype(bf16)

    def deltas(b, _):
        spot_b = place(b)
        prod = g_ref[pl.ds(spot_b, blk), :].astype(f32) * att_ref[pl.ds(spot_b, blk), :].astype(f32)
        high = prod.astype(bf16)
        low = (prod - high.astype(f32)).astype(bf16)
        delta_ref[b] = (lax.dot_general(pick, high, NT, preferred_element_type=f32)
                        + lax.dot_general(pick, low, NT, preferred_element_type=f32))
        return 0
    lax.fori_loop(0, nb, deltas, 0)

    lane_lo = lax.broadcasted_iota(jnp.int32, (blk, 128), 1) < HEAD
    count = count_ref[0]

    def block(kb, qb, masked):
        k_at, q_at = place(kb), place(qb)
        if masked:
            keep = (lax.broadcasted_iota(jnp.int32, (blk, blk), 0)
                    <= lax.broadcasted_iota(jnp.int32, (blk, blk), 1))
        else:
            apart = jnp.where(kb * count // nb == qb * count // nb, 0.0, 1e30)
        for pr in range(width // 128):
            cols = [pl.ds(j * width + 128 * pr, 128) for j in range(3)]
            q = qkv_ref[pl.ds(q_at, blk), cols[0]]
            g = g_ref[pl.ds(q_at, blk), cols[0]]
            k = qkv_ref[pl.ds(k_at, blk), cols[1]]
            v = qkv_ref[pl.ds(k_at, blk), cols[2]]
            dk = dv = dq = None
            for h in range(2):
                mine = lane_lo if h == 0 else ~lane_lo
                head = 2 * pr + h
                kh = jnp.where(mine, k, bf16(0))
                vh = jnp.where(mine, v, bf16(0))
                s = lax.dot_general(kh, q, NT, preferred_element_type=f32) * LOG2E
                lse = lse_ref[qb, pl.ds(head, 1), :]
                if not masked:
                    lse = lse + apart
                e = jnp.exp2(s - lse)
                if masked:
                    e = jnp.where(keep, e, 0.0)
                dp = lax.dot_general(vh, g, NT, preferred_element_type=f32)
                ds = (e * (dp - delta_ref[qb, pl.ds(head, 1), :])).astype(bf16)
                e = e.astype(bf16)
                dv1 = jnp.dot(e, jnp.where(mine, g, bf16(0)), preferred_element_type=f32)
                dk1 = jnp.dot(ds, jnp.where(mine, q, bf16(0)), preferred_element_type=f32)
                dq1 = lax.dot_general(ds, kh, TN, preferred_element_type=f32)
                dk, dv, dq = (dk1, dv1, dq1) if h == 0 else (dk + dk1, dv + dv1, dq + dq1)
            if masked:
                dk_ref[:, cols[0]] = dk
                dv_ref[:, cols[0]] = dv
            else:
                dk_ref[:, cols[0]] += dk
                dv_ref[:, cols[0]] += dv
            dq_ref[pl.ds(q_at, blk), cols[0]] += dq

    pairs = nb * (nb + 1) // 2
    early = n

    def ticks(lo, hi):
        def one(k, _):
            @pl.when(k == 0)
            def _():
                gl_copy.wait()
                core_copy.wait()
            tick(k)
            return 0
        lax.fori_loop(lo, hi, one, 0)

    def small_ticks(i):
        for b in range(bits + 1):
            @pl.when(i == b + 1)
            def _(b=b):
                small_end(b)
                if b < bits:
                    small_start(b + 1)

    def key_block(kb, i):
        small_ticks(i)
        ticks(i * early // pairs, (i + 1) * early // pairs)
        block(kb, kb, True)

        def other(qb, i):
            small_ticks(i)
            ticks(i * early // pairs, (i + 1) * early // pairs)
            block(kb, qb, False)
            return i + 1
        i = lax.fori_loop(kb + 1, nb, other, i + 1)
        k_at = place(kb)
        for j, part in ((0, dq_ref[pl.ds(k_at, blk), :] * 0.125), (1, dk_ref[...]), (2, dv_ref[...])):
            low = part.astype(bf16)
            qkv_ref[pl.ds(k_at, blk), pl.ds(j * width, width)] = low
            if j != 1:
                hb_ref[j // 2] += jnp.sum(low.astype(f32), axis=0, keepdims=True)
        return i
    done = lax.fori_loop(0, nb, key_block, 0)
    for b in range(bits + 1):
        if b + 1 >= pairs:
            small_end(b)
            if b < bits:
                small_start(b + 1)
    v, r = vb_ref[bits], rb_ref[bits]
    small_out[...] = v + jnp.concatenate([r[0:4], r[6:8], r[6:8]])

    for copy in w_copies:
        copy.wait()
    piece = half // 4

    def da_copy(i):
        return put(dsend_ref.at[i], drecv_ref.at[i], d_send.at[i], d_recv.at[i], "peer")

    def send_rows(i, _):
        gq = qkv_ref[pl.ds(pl.multiple_of(half + i * piece, piece), piece), :]
        dsend_ref[i] = lax.dot_general(gq, w_ref[...], NT, preferred_element_type=f32).astype(bf16)
        da_copy(i).start()
        return 0
    lax.fori_loop(0, 4, send_rows, 0)

    def head_grads(i, _):
        at = pl.ds(pl.multiple_of(i * 384, 384), 384)
        acc = (lax.dot_general(own_ref[:, at], qkv_ref[pl.ds(0, half), :], TN, preferred_element_type=f32)
               + lax.dot_general(oth_ref[:, at], qkv_ref[pl.ds(half, half), :], TN, preferred_element_type=f32))
        for j in range(3):
            cut = acc[:, j * width:(j + 1) * width].reshape(384 // ch2, ch2, width).astype(bf16)
            t_ref[pl.ds((j * dim + i * 384) // ch2, 384 // ch2)] = cut
        return 0
    lax.fori_loop(0, dim // 384, head_grads, 0)
    gx_copy.wait()
    tcore_copy = put(t_ref.at[pl.ds((1 - core) * n, n)], tmate_ref.at[0], tc_sem.at[0], tc_sem.at[1], "mate")
    tcore_copy.start()

    def own_rows(i, _):
        at = pl.ds(pl.multiple_of(i * piece, piece), piece)
        da_ref[at, :] = lax.dot_general(qkv_ref[at, :], w_ref[...], NT, preferred_element_type=f32)
        return 0
    lax.fori_loop(0, 4, own_rows, 0)
    tcore_copy.wait()

    def tail_ticks(lo, hi):
        def one(k, _):
            ttick(k)
            return 0
        lax.fori_loop(lo, hi, one, 0)

    sums = jnp.zeros((2, dim), f32)
    ub_ref[0] = jnp.zeros((8, dim), f32)
    for i in range(4):
        ticks(early + i * n // 4, early + (i + 1) * n // 4)
        tail_ticks(i * n // 4, (i + 1) * n // 4)
        da_copy(i).wait()

        def norm_rows(j, _, i=i):
            inner = piece // 4
            at = pl.ds(pl.multiple_of(i * piece + j * inner, inner), inner)
            x = tok_ref[at, :].astype(f32)
            x = x - jnp.mean(x, axis=-1, keepdims=True)
            inv = lax.rsqrt(jnp.mean(x * x, axis=-1, keepdims=True) + EPSILON)
            h = x * inv
            e = da_ref[at, :] + drecv_ref[i, pl.ds(pl.multiple_of(j * inner, inner), inner), :].astype(f32)
            eg = e * gain_ref[...]
            back = inv * (eg - jnp.mean(eg, axis=-1, keepdims=True)
                          - h * jnp.mean(eg * h, axis=-1, keepdims=True))
            gtok_ref[at, :] = (gm_ref[at, :] + back).astype(bf16)
            ub_ref[0, 0:1, :] += jnp.sum(e * h, axis=0, keepdims=True)
            ub_ref[0, 1:2, :] += jnp.sum(e, axis=0, keepdims=True)
            return 0
        lax.fori_loop(0, 4, norm_rows, 0)
    ub_ref[0, 2:3, pl.ds(0, width)] = hb_ref[0]
    ub_ref[0, 2:3, pl.ds(width, width)] = hb_ref[1]
    last_copies = []
    for b in range(bits + 1):
        copy = small_copy(ub_ref, qb_ref, u_send, u_recv, b)
        copy.start()
        tail_ticks(n + b * n // (bits + 1), n + (b + 1) * n // (bits + 1))
        copy.wait()
        if b < bits:
            ub_ref[b + 1] = ub_ref[b] + qb_ref[b]
    v, r = ub_ref[bits], qb_ref[bits]
    last_out[...] = jnp.concatenate([v[0:2] + r[0:2], v[2:8]])
    finish()
    tfinish()


def backward(size, count, qkv, att, gown, goth, lse, gw, a1, a1_other, w, gmix, small, tokens, gain, grad_middle,
             blk=512):
    rows, total = qkv.shape
    width = total // 3
    half, dim = tokens.shape
    nb = rows // blk
    n = size // 2
    bits = size.bit_length() - 1
    hidden = gw.shape[2]
    gw = gw.reshape(2, 2, n, hidden // n, dim)
    ch, ch2 = hidden // n, 4 * dim // (2 * n)
    gmix = gmix.reshape(dim // ch2, ch2, width)
    vm = pl.BlockSpec(memory_space=pltpu.VMEM)
    hb = pl.BlockSpec(memory_space=pl.ANY)
    sm = pl.BlockSpec(memory_space=pltpu.SMEM)
    V, S = pltpu.VMEM, pltpu.SemaphoreType.DMA
    return pl.pallas_call(
        functools.partial(backward_kernel, size, blk),
        in_specs=[sm, hb, vm, hb, hb, vm, hb, vm, vm, hb, hb, vm, vm, vm, vm],
        out_specs=[vm] * 5,
        out_shape=[jax.ShapeDtypeStruct((2 * n, ch, dim), bf16),
                   jax.ShapeDtypeStruct((2 * n, ch2, width), bf16),
                   jax.ShapeDtypeStruct((half, dim), bf16),
                   jax.ShapeDtypeStruct((8, dim), f32),
                   jax.ShapeDtypeStruct((8, dim), f32)],
        scratch_shapes=[
            V((rows, total), bf16), V((rows, width), bf16), V((nb, 8, blk), f32), V((rows, width), f32),
            V((blk, width), f32), V((blk, width), f32), V((dim, total), bf16),
            V((2, n, ch, dim), bf16), V((2, n, ch, dim), bf16), V((n - 1, 2, ch, dim), bf16), V((2, ch, dim), bf16),
            V((ch, dim), bf16),
            V((2 * n, ch2, width), bf16), V((1, n, ch2, width), bf16), V((n - 1, 1, ch2, width), bf16),
            V((1, ch2, width), bf16),
            V((half, dim), f32), V((4, half // 4, dim), bf16), V((4, half // 4, dim), bf16),
            V((bits + 1, 8, dim), f32), V((bits + 1, 8, dim), f32), V((bits + 1, 8, dim), f32),
            V((bits + 1, 8, dim), f32), V((2, 1, width), f32),
            S((8,)), S((2,)), S((n - 1,)), S((n - 1,)), S((n - 1,)), S((n - 1,)), S((n,)), S((n,)), S((2,)),
            S((2,)), S((n - 1,)), S((n - 1,)), S((n - 1,)), S((n - 1,)), S((n,)), S((n,)),
            S((4,)), S((4,)), S((bits + 1,)), S((bits + 1,)), S((bits + 1,)), S((bits + 1,))],
        compiler_params=pltpu.CompilerParams(collective_id=0, has_side_effects=True,
                                             vmem_limit_bytes=67_043_328),
        cost_estimate=pl.CostEstimate(flops=40_000_000_000, transcendentals=0, bytes_accessed=30_000_000),
        name="backward",
    )(count, qkv, att, gown, goth, lse, gw, a1, a1_other, w, gmix, small, tokens, gain, grad_middle)


def to_peer(v):
    return lax.ppermute(v, "tensor", SWAP)


def row_stats(v):
    centre = jnp.mean(v, axis=-1, keepdims=True)
    centred = v - centre
    inv = lax.rsqrt(jnp.mean(centred * centred, axis=-1, keepdims=True) + EPSILON)
    return centre, inv


def norm_back(e, gain, h, inv):
    eg = e * gain
    return inv * (eg - jnp.mean(eg, axis=-1, keepdims=True)
                  - h * jnp.mean(eg * h, axis=-1, keepdims=True))


def add16(a, b):
    return (a.astype(f32) + b.astype(f32)).astype(bf16)


def dot32(a, b):
    return jnp.dot(a, b, preferred_element_type=f32)


def dot_nt(a, b):
    return lax.dot_general(a, b, NT, preferred_element_type=f32)


def dot_tn(a, b):
    return lax.dot_general(a, b, TN, preferred_element_type=f32)


def xor_step(v, size, bit):
    return lax.ppermute(v, "dp", [(i, i ^ (1 << bit)) for i in range(size)])


def gelu_pair(v):
    t = jnp.tanh(GELU_C * (v + 0.044715 * v * v * v))
    return 0.5 * v * (1.0 + t), 0.5 * (1.0 + t) + 0.5 * v * (1.0 - t * t) * (
        GELU_C * (1.0 + 3.0 * 0.044715 * v * v))


def local(
    tokens,
    seq_count,
    first_gain,
    first_shift,
    heads_weight,
    heads_bias,
    mixing_weight,
    mixing_bias,
    second_gain,
    second_shift,
    up_weight,
    up_bias,
    down_weight,
    down_bias,
    cotangent,
):
    size = lax.axis_size("dp")
    me = lax.axis_index("dp")
    side = lax.axis_index("tensor")
    info = jnp.stack([side.astype(jnp.int32), seq_count[0]])
    half, dim = tokens.shape
    width = heads_weight.shape[2]
    hidden = up_weight.shape[1]

    pu, pd, pm = dim // size, hidden // size, width // size
    piece = jnp.concatenate([
        lax.dynamic_slice(up_weight, (me * pu, 0), (pu, hidden // 2)),
        lax.dynamic_slice(up_weight, (me * pu, hidden // 2), (pu, hidden // 2)),
        lax.dynamic_slice_in_dim(down_weight, me * pd, pd, 0),
        lax.dynamic_slice_in_dim(mixing_weight, me * pm, pm, 0)])
    piece = to_peer(piece)
    up_bias_other = to_peer(up_bias)

    x = tokens.astype(f32)
    centre1, inv1 = row_stats(x)
    a1 = ((x - centre1) * inv1 * first_gain + first_shift).astype(bf16)
    piece, a1 = lax.optimization_barrier((piece, a1))
    a1_other = to_peer(a1)
    packed = lax.all_gather(piece, "dp", axis=0)
    up_other = jnp.concatenate([packed[:, :pu].reshape(dim, hidden // 2),
                                packed[:, pu:2 * pu].reshape(dim, hidden // 2)], axis=1)
    down_other = packed[:, 2 * pu:2 * pu + pd].reshape(hidden, dim)
    mix_other = packed[:, 2 * pu + pd:].reshape(width, dim)
    bias3 = jnp.stack([heads_bias[0], jnp.zeros_like(heads_bias[0]), heads_bias[1]])
    qkv, att, lse = attn_forward(info, a1, a1_other, heads_weight, bias3)
    att_mine = att[:half]
    att_recv = to_peer(att[half:])
    middle = x + BRANCH * (dot32(att_mine, mixing_weight) + dot32(att_recv, mix_other) + mixing_bias)
    centre2, inv2 = row_stats(middle)
    h2 = (middle - centre2) * inv2
    a2 = (h2 * second_gain + second_shift).astype(bf16)

    g_out = cotangent.astype(f32)
    grad_mlp = (BRANCH * g_out).astype(bf16)
    down_sum = 0.0
    grad_a2 = 0.0
    grads_up, grads_down, bias_up = [], [], []
    for up, bias, down in ((up_weight, up_bias, down_weight), (up_other, up_bias_other, down_other)):
        pre = dot32(a2, up) + bias
        act, slope = gelu_pair(pre)
        act = act.astype(bf16)
        down_sum += dot32(act, down)
        grad_pre = (dot_nt(grad_mlp, down) * slope).astype(bf16)
        grads_down.append(dot_tn(act, grad_mlp).astype(bf16))
        grads_up.append(jnp.concatenate([dot_tn(a2, grad_pre[:, :hidden // 2]),
                                         dot_tn(a2, grad_pre[:, hidden // 2:])]).astype(bf16))
        bias_up.append(jnp.sum(grad_pre, axis=0, dtype=f32).reshape(2, dim))
        grad_a2 += dot_nt(grad_pre, up)
    result = (middle + BRANCH * (down_sum + down_bias)).astype(bf16)
    grads = jnp.stack([jnp.stack(grads_down), jnp.stack(grads_up)])

    grad_middle = g_out + norm_back(grad_a2, second_gain, h2, inv2)
    grad_attn = (BRANCH * grad_middle).astype(bf16)
    g_own = dot_nt(grad_attn, mixing_weight).astype(bf16)
    g_other = to_peer(dot_nt(grad_attn, mix_other).astype(bf16))
    small = jnp.concatenate([
        jnp.stack([BRANCH * jnp.sum(g_out, axis=0), jnp.sum(grad_a2 * h2, axis=0),
                   jnp.sum(grad_a2, axis=0), BRANCH * jnp.sum(grad_middle, axis=0)])] + bias_up)
    grad_mix = add16(dot_tn(att_mine, grad_attn), to_peer(dot_tn(att_recv, grad_attn).astype(bf16)))

    grad_mix = jnp.concatenate([grad_mix[:, :width], grad_mix[:, width:]])
    fin, tail, grad_tokens, small, last = backward(
        size, seq_count, qkv, att, g_own, g_other, lse, grads, a1, a1_other, heads_weight, grad_mix, small,
        tokens, first_gain[None], grad_middle)
    groups = 1.0 / size
    small = small * groups
    last = last * groups
    fin = fin.reshape(2, hidden, dim).astype(f32) * groups
    tail = tail.reshape(4 * dim, width).astype(f32) * groups
    grad_up = fin[1]
    return (
        result,
        grad_tokens,
        last[0],
        last[1],
        tail[:3 * dim].reshape(3, dim, width),
        last[2].reshape(2, width),
        jnp.concatenate([tail[3 * dim:3 * dim + width], tail[3 * dim + width:]], axis=1),
        small[3],
        small[1],
        small[2],
        jnp.concatenate([grad_up[:dim], grad_up[dim:]], axis=1),
        small[4:6].reshape(hidden),
        fin[0],
        small[0],
    )


def solution(mesh):
    placed = (
        P(("dp", "tensor"), None),
        P("dp"),
        P(),
        P(),
        P(None, None, "tensor"),
        P(None, "tensor"),
        P("tensor", None),
        P(),
        P(),
        P(),
        P(None, "tensor"),
        P("tensor"),
        P("tensor", None),
        P(),
        P(("dp", "tensor"), None),
    )
    return jax.shard_map(
        local,
        mesh=mesh,
        in_specs=placed,
        out_specs=(
            P(("dp", "tensor"), None),
            P(("dp", "tensor"), None),
            P(),
            P(),
            P(None, None, "tensor"),
            P(None, "tensor"),
            P("tensor", None),
            P(),
            P(),
            P(),
            P(None, "tensor"),
            P("tensor"),
            P("tensor", None),
            P(),
        ),
        check_vma=False,
    )
```

```python
import functools, math
import jax
import jax.numpy as jnp
from jax import lax
from jax.experimental import pallas as pl
from jax.experimental.pallas import tpu as pltpu
from jax.sharding import PartitionSpec as P

HEAD = 64
DEPTH = 12
EPSILON = 1e-05
BRANCH = 1.0 / math.sqrt(DEPTH)
GELU_C = math.sqrt(2.0 / math.pi)
SWAP = ((0, 1), (1, 0))
LOG2E = math.log2(math.e)
NT = (((1,), (1,)), ((), ()))
TN = (((0,), (0,)), ((), ()))
f32 = jnp.float32
bf16 = jnp.bfloat16


def attn_forward_kernel(blk, info, own_ref, oth_ref, w_ref, b_ref, qkv_ref, att_ref, lse_ref, acc_ref, top_ref):
    qb = pl.program_id(0)
    nb = pl.num_programs(0)
    half = own_ref.shape[0]
    width = w_ref.shape[2]
    side, count = info[0], info[1]

    @pl.when(qb == 0)
    def _():
        step = 256
        for part, ref in enumerate((own_ref, oth_ref)):
            def rows_loop(i, _, part=part, ref=ref):
                rows = ref[pl.ds(pl.multiple_of(i * step, step), step), :]
                to = pl.multiple_of(part * half + i * step, step)
                for j in range(3):
                    y = jnp.dot(rows, w_ref[j], preferred_element_type=f32) + b_ref[pl.ds(j, 1), :]
                    y = y.astype(bf16)
                    if j == 0:
                        y = y * bf16(0.125)
                    qkv_ref[pl.ds(to, step), pl.ds(j * width, width)] = y
                return 0
            lax.fori_loop(0, half // step, rows_loop, 0)

    def place(b):
        return pl.multiple_of(lax.rem(b + side * (nb // 2), nb) * blk, blk)

    lane_lo = lax.broadcasted_iota(jnp.int32, (blk, 128), 1) < HEAD
    first = (qb * count // nb) * nb // count
    q_at = place(qb)

    def block(kb, fresh, masked):
        k_at = place(kb)
        if masked:
            qi = lax.broadcasted_iota(jnp.int32, (blk, blk), 0)
            ki = lax.broadcasted_iota(jnp.int32, (blk, blk), 1)
            keep = ki <= qi
        for p in range(width // 128):
            q = qkv_ref[pl.ds(q_at, blk), pl.ds(0 * width + 128 * p, 128)]
            k = qkv_ref[pl.ds(k_at, blk), pl.ds(1 * width + 128 * p, 128)]
            v = qkv_ref[pl.ds(k_at, blk), pl.ds(2 * width + 128 * p, 128)]
            for h in range(2):
                mine = lane_lo if h == 0 else ~lane_lo
                head = 2 * p + h
                qh = jnp.where(mine, q, bf16(0))
                vh = jnp.where(mine, v, bf16(1))
                s = lax.dot_general(qh, k, NT, preferred_element_type=f32) * LOG2E
                if masked:
                    s = jnp.where(keep, s, -1e30)
                top = jnp.max(s, axis=1, keepdims=True)
                if fresh:
                    e = jnp.exp2(s - top)
                    acc_ref[head] = jnp.dot(e.astype(bf16), vh, preferred_element_type=f32)
                    top_ref[head] = jnp.broadcast_to(top, (blk, 128))
                else:
                    old = top_ref[head]
                    new = jnp.maximum(old, top)
                    e = jnp.exp2(s - new[:, :1])
                    acc_ref[head] = acc_ref[head] * jnp.exp2(old - new) + jnp.dot(
                        e.astype(bf16), vh, preferred_element_type=f32)
                    top_ref[head] = new

    block(qb, True, True)

    def loop(kb, _):
        block(kb, False, False)
        return 0
    lax.fori_loop(first, qb, loop, 0)

    for p in range(width // 128):
        a0, a1 = acc_ref[2 * p], acc_ref[2 * p + 1]
        num = jnp.where(lane_lo, a0, a1)
        den = jnp.where(lane_lo, pltpu.roll(a0, HEAD, 1), pltpu.roll(a1, HEAD, 1))
        att_ref[pl.ds(q_at, blk), pl.ds(128 * p, 128)] = (num / den).astype(bf16)
        logs = jnp.where(lane_lo, top_ref[2 * p], top_ref[2 * p + 1]) + jnp.log2(den)
        rows = logs.T
        lse_ref[qb, pl.ds(2 * p, 1), :] = rows[0:1]
        lse_ref[qb, pl.ds(2 * p + 1, 1), :] = rows[HEAD:HEAD + 1]


def attn_forward(info, own, oth, w, b, blk=512):
    half = own.shape[0]
    rows = 2 * half
    width = w.shape[2]
    nb = rows // blk
    heads = width // HEAD
    vm = pl.BlockSpec(memory_space=pltpu.VMEM)
    return pl.pallas_call(
        functools.partial(attn_forward_kernel, blk),
        grid=(nb,),
        in_specs=[pl.BlockSpec(memory_space=pltpu.SMEM), vm, vm, vm, vm],
        out_specs=[vm, vm, vm],
        out_shape=[jax.ShapeDtypeStruct((rows, 3 * width), bf16),
                   jax.ShapeDtypeStruct((rows, width), bf16),
                   jax.ShapeDtypeStruct((nb, 8, blk), f32)],
        scratch_shapes=[pltpu.VMEM((heads, blk, 128), f32), pltpu.VMEM((heads, blk, 128), f32)],
        compiler_params=pltpu.CompilerParams(vmem_limit_bytes=56 << 20),
        cost_estimate=pl.CostEstimate(flops=12_000_000_000, transcendentals=0, bytes_accessed=12_000_000),
        name="attn_forward",
    )(info, own, oth, w, b)


def remote(src, dst, send, recv, where):
    return pltpu.make_async_remote_copy(src_ref=src, dst_ref=dst, send_sem=send, recv_sem=recv,
                                        device_id=where, device_id_type=pl.DeviceIdType.MESH)


def ring_sum(n, lanes, pos, where, local, mate, slot, first, send, recv):
    def hop(src, s, u):
        return remote(src, slot(s, u), send.at[s * lanes + u], recv.at[s * lanes + u], where)

    def at(c):
        return lax.rem(c + 2 * n, n)

    def tick(k, u):
        @pl.when(k == 0)
        def _():
            c = at(pos)
            first(u)[...] = (local(c, u)[...].astype(f32) + mate(c, u)[...].astype(f32)).astype(bf16)
            hop(first(u), 0, u).start()

        @pl.when(k > 0)
        def _():
            c = at(pos - k)
            here = slot(k - 1, u)
            hop(here, k - 1, u).wait_recv()
            here[...] = (here[...].astype(f32) + local(c, u)[...].astype(f32)
                         + mate(c, u)[...].astype(f32)).astype(bf16)

            @pl.when(k < n - 1)
            def _():
                hop(here, k, u).start()

    def finish():
        def one(s, _):
            for u in range(lanes):
                hop(slot(s, u), s, u).wait_send()
            return 0
        lax.fori_loop(0, n - 1, one, 0)
    return tick, finish


def ring_spread(n, lanes, pos, core, where, mate, view, send, recv, m_send, m_recv):
    def spot(c):
        return core * n + lax.rem(c + 2 * n, n)

    def hop(s, u):
        chunk = view(spot(pos + 1 - s), u)
        return remote(chunk, chunk, send.at[s * lanes + u], recv.at[s * lanes + u], where)

    def over(s, u):
        chunk = view(spot(pos + 1 - s), u)
        return remote(chunk, chunk, m_send.at[s * lanes + u], m_recv.at[s * lanes + u], mate)

    def tick(k, u):
        @pl.when(k > 0)
        def _():
            hop(k - 1, u).wait_recv()

        @pl.when(k < n - 1)
        def _():
            hop(k, u).start()
        over(k, u).start()

    def finish():
        def one(s, _):
            for u in range(lanes):
                @pl.when(s < n - 1)
                def _():
                    hop(s, u).wait_send()
                over(s, u).wait()
            return 0
        lax.fori_loop(0, n, one, 0)
    return tick, finish


def backward_kernel(size, blk, count_ref, qkv_hbm, att_ref, arecv_ref, lse_ref, gd_hbm, gu_hbm, own_hbm, oth_hbm,
                    w_hbm, mix_ref, mixo_ref, small_ref, tok_hbm, gain1_ref, gain2_ref, cot_hbm, mid_hbm, da2_hbm,
                    fin_ref, tail_ref, gtok_hbm, small_out, last_out,
                    qkv_ref, g_ref, delta_ref, dq_ref, dk_ref, dv_ref, w_ref, gm_ref, gsend_ref, row_ref,
                    gl_ref, mate_ref, slot_ref, first_ref, yin_ref,
                    t_ref, tmate_ref, tslot_ref, tfirst_ref, xsend_ref, xrecv_ref,
                    da_ref, dsend_ref, drecv_ref, vb_ref, rb_ref, ub_ref, qb_ref, hb_ref,
                    in_sem, c_sem, s_send, s_recv, a_send, a_recv, m_send, m_recv, y_sem,
                    tc_sem, ts_send, ts_recv, ta_send, ta_recv, tm_send, tm_recv,
                    d_send, d_recv, v_send, v_recv, u_send, u_recv, g_send, g_recv, x_sem, o_sem):
    n = size // 2
    bits = size.bit_length() - 1
    rows, total = qkv_ref.shape
    half = rows // 2
    width = total // 3
    dim = w_hbm.shape[1]
    nb = rows // blk
    me, side = lax.axis_index("dp"), lax.axis_index("tensor")
    core, chip = lax.rem(me, 2), me // 2
    odd = lax.rem(chip, 2)
    p = (1 - odd) * (chip // 2) + odd * (n - 1 - chip // 2)

    def chip_at(q):
        up = q // (n // 2)
        return (1 - up) * 2 * q + up * (2 * (n - 1 - q) + 1)
    pos = (1 - core) * p + core * lax.rem(n - p, n)
    step = 1 - 2 * core
    follow = {"dp": 2 * chip_at(lax.rem(p + step + n, n)) + core}
    before = {"dp": 2 * chip_at(lax.rem(p - step + n, n)) + core}
    mate = {"dp": me + 1 - 2 * core}
    peer = {"tensor": 1 - side}
    partner = [mate] + [{"dp": me + (1 - 2 * lax.rem(me // (1 << b), 2)) * (1 << b)} for b in range(1, bits)] + [peer]

    def fetch(src, dst, i):
        copy = pltpu.make_async_copy(src, dst, in_sem.at[i])
        copy.start()
        return copy
    da2_copy = fetch(da2_hbm, da_ref, 0)
    mid_copy = fetch(mid_hbm, dq_ref, 1)
    cot_copy = fetch(cot_hbm, row_ref, 7)
    gl_copies = [pltpu.make_async_copy(src, gl_ref, in_sem.at[2]) for src in (gd_hbm, gu_hbm)]
    for which in range(2):
        pl.when(core == which)(gl_copies[which].start)
    q_copy = fetch(qkv_hbm, qkv_ref, 3)
    w_copies = [fetch(w_hbm.at[j], w_ref.at[:, pl.ds(j * width, width)], 4 + j) for j in range(3)]
    ch2 = t_ref.shape[1]

    barrier = pltpu.get_barrier_semaphore()
    friends = [follow, before] + partner
    for to in friends:
        pl.semaphore_signal(barrier, inc=1, device_id=to, device_id_type=pl.DeviceIdType.MESH)
    pl.semaphore_wait(barrier, len(friends))

    core_copies = [remote(src, mate_ref, c_sem.at[0], c_sem.at[1], mate) for src in (gu_hbm, gd_hbm)]
    for which in range(2):
        pl.when(core == which)(core_copies[which].start)

    rs_tick, rs_finish = ring_sum(
        n, 2, pos, follow, lambda c, u: gl_ref.at[1 - u, c], lambda c, u: mate_ref.at[1 - u, c],
        lambda s, u: slot_ref.at[s, 1 - u], lambda u: first_ref.at[1 - u], s_send, s_recv)
    cut = dim // 2

    def fin_view(c, u):
        return fin_ref.at[c, :, pl.ds(pl.multiple_of(u * cut, 128), cut)]
    ag_tick, ag_finish = ring_spread(n, 2, pos, core, follow, mate, fin_view, a_send, a_recv, m_send, m_recv)
    y_copy = remote(slot_ref.at[n - 2, 1], yin_ref, y_sem.at[0], y_sem.at[1], peer)

    def tick(q):
        @pl.when(q == 0)
        def _():
            gl_copies[0].wait()
            core_copies[0].wait()

        @pl.when(q < 2 * n)
        def _():
            rs_tick(q // 2, lax.rem(q, 2))

            @pl.when(q == 2 * n - 2)
            def _():
                y_copy.start()

        @pl.when(q == 2 * n)
        def _():
            y_copy.wait()
            fin_ref[core * n + lax.rem(pos + 1, n)] = (slot_ref[n - 2, 0].astype(f32)
                                                       + yin_ref[...].astype(f32)).astype(bf16)

        @pl.when(q > 2 * n)
        def _():
            r = q - 2 * n - 1
            ag_tick(r // 2, lax.rem(r, 2))
    q_rs, q_all = 2 * n + 1, 4 * n + 1

    def ticks(lo, hi):
        def one(k, _):
            tick(k)
            return 0
        lax.fori_loop(lo, hi, one, 0)

    piece = half // 4
    vb_ref[0] = small_ref[...]
    da2_copy.wait()
    mid_copy.wait()
    cot_copy.wait()
    inner = piece // 4

    def g_copy(i):
        return remote(gsend_ref.at[i], g_ref.at[pl.ds(pl.multiple_of(half + i * piece, piece), piece)],
                      g_send.at[i], g_recv.at[i], peer)

    def second_norm(i, _):
        def norm_rows(j, _):
            to = pl.multiple_of(j * inner, inner)
            at = pl.ds(pl.multiple_of(i * piece + j * inner, inner), inner)
            x = dq_ref[at, :]
            x = x - jnp.mean(x, axis=-1, keepdims=True)
            inv = lax.rsqrt(jnp.mean(x * x, axis=-1, keepdims=True) + EPSILON)
            h = x * inv
            e = da_ref[at, :]
            eg = e * gain2_ref[...]
            g_out = row_ref[at, :].astype(f32)
            gm = g_out + inv * (eg - jnp.mean(eg, axis=-1, keepdims=True)
                                - h * jnp.mean(eg * h, axis=-1, keepdims=True))
            gm_ref[at, :] = gm
            dsend_ref[i, pl.ds(to, inner), :] = (BRANCH * gm).astype(bf16)
            vb_ref[0, 0:1, :] += BRANCH * jnp.sum(g_out, axis=0, keepdims=True)
            vb_ref[0, 1:2, :] += jnp.sum(e * h, axis=0, keepdims=True)
            vb_ref[0, 2:3, :] += jnp.sum(e, axis=0, keepdims=True)
            vb_ref[0, 3:4, :] += BRANCH * jnp.sum(gm, axis=0, keepdims=True)
            return 0
        lax.fori_loop(0, 4, norm_rows, 0)
        ga = dsend_ref[i]
        gsend_ref[i] = dot_nt(ga, mixo_ref[...]).astype(bf16)
        g_copy(i).start()
        return 0
    lax.fori_loop(0, 4, second_norm, 0)
    tok_copy = fetch(tok_hbm, row_ref, 8)

    def small_copy(buf, inbox, send, recv, b):
        return remote(buf.at[b], inbox.at[b], send.at[b], recv.at[b], partner[b])

    def small_start(b):
        small_copy(vb_ref, rb_ref, v_send, v_recv, b).start()

    def small_end(b):
        small_copy(vb_ref, rb_ref, v_send, v_recv, b).wait()
        if b < bits:
            vb_ref[b + 1] = vb_ref[b] + rb_ref[b]
    small_start(0)

    pre = 6 * n // 8
    ticks(0, pre // 3)
    for i in range(4):
        g_ref[pl.ds(i * piece, piece), :] = dot_nt(dsend_ref[i], mix_ref[...]).astype(bf16)

    def mix_grad(lhs_ref):
        acc = jnp.zeros((width, dim), f32)
        for i in range(4):
            acc += dot_tn(lhs_ref[pl.ds(i * piece, piece), :], dsend_ref[i])
        return acc
    first_mix = 3 * dim // ch2
    acc = mix_grad(arecv_ref)
    for i in range(2):
        xsend_ref[i] = acc[:, i * width:(i + 1) * width].astype(bf16)
    x_copy = remote(xsend_ref, xrecv_ref, x_sem.at[0], x_sem.at[1], peer)
    ticks(pre // 3, 2 * pre // 3)
    acc = mix_grad(att_ref)

    def mix_place(i):
        return pl.ds(first_mix + i * (width // ch2), width // ch2)
    for i in range(2):
        t_ref[mix_place(i)] = acc[:, i * width:(i + 1) * width].reshape(width // ch2, ch2, width).astype(bf16)
    hb_ref[...] = jnp.zeros_like(hb_ref)
    dq_ref[...] = jnp.zeros_like(dq_ref)
    q_copy.wait()
    ticks(2 * pre // 3, pre)
    for i in range(4):
        g_copy(i).wait()
    x_copy.start()

    def local_block(b):
        return lax.rem(b + side * (nb // 2), nb)

    def place(b):
        return pl.multiple_of(local_block(b) * blk, blk)

    def dq_at(b):
        spot = local_block(b)
        return (pl.ds(pl.multiple_of(lax.rem(spot, nb // 2) * blk, blk), blk),
                pl.multiple_of(spot // (nb // 2) * width, 128))
    pick = (lax.broadcasted_iota(jnp.int32, (8, width), 1) // HEAD
            == lax.broadcasted_iota(jnp.int32, (8, width), 0)).astype(bf16)

    def deltas(b, _):
        at = pl.ds(place(b), blk)
        prod = g_ref[at, :].astype(f32) * att_ref[at, :].astype(f32)
        high = prod.astype(bf16)
        low = (prod - high.astype(f32)).astype(bf16)
        delta_ref[b] = dot_nt(pick, high) + dot_nt(pick, low)
        return 0
    lax.fori_loop(0, nb, deltas, 0)

    lane_lo = lax.broadcasted_iota(jnp.int32, (blk, 128), 1) < HEAD
    count = count_ref[0]
    groups = width // 128
    slots = groups * nb * (nb + 1) // 2
    slow = 11 * slots // 15
    q_mid = q_rs + (q_all - q_rs) // 2

    def tick_mark(i):
        early = pre + i * (q_rs - pre) // slow
        late = q_rs + (i - slow) * (q_mid - q_rs) // (slots - slow)
        return jnp.where(i < slow, early, late)

    def block(kb, qb, masked, i):
        k_at, q_at = place(kb), place(qb)
        dq_rows, dq_lane = dq_at(qb)
        if masked:
            keep = (lax.broadcasted_iota(jnp.int32, (blk, blk), 0)
                    <= lax.broadcasted_iota(jnp.int32, (blk, blk), 1))
        else:
            apart = jnp.where(kb * count // nb == qb * count // nb, 0.0, 1e30)
        for pr in range(groups):
            ticks(tick_mark(i + pr), tick_mark(i + pr + 1))
            cols = [pl.ds(j * width + 128 * pr, 128) for j in range(3)]
            q = qkv_ref[pl.ds(q_at, blk), cols[0]]
            g = g_ref[pl.ds(q_at, blk), cols[0]]
            k = qkv_ref[pl.ds(k_at, blk), cols[1]]
            v = qkv_ref[pl.ds(k_at, blk), cols[2]]
            dk = dv = dq = None
            for h in range(2):
                mine = lane_lo if h == 0 else ~lane_lo
                head = 2 * pr + h
                kh = jnp.where(mine, k, bf16(0))
                vh = jnp.where(mine, v, bf16(0))
                s = dot_nt(kh, q) * LOG2E
                lse = lse_ref[qb, pl.ds(head, 1), :]
                if not masked:
                    lse = lse + apart
                e = jnp.exp2(s - lse)
                if masked:
                    e = jnp.where(keep, e, 0.0)
                dp = dot_nt(vh, g)
                ds = (e * (dp - delta_ref[qb, pl.ds(head, 1), :])).astype(bf16)
                e = e.astype(bf16)
                dv1 = dot32(e, jnp.where(mine, g, bf16(0)))
                dk1 = dot32(ds, jnp.where(mine, q, bf16(0)))
                dq1 = dot_tn(ds, kh)
                dk, dv, dq = (dk1, dv1, dq1) if h == 0 else (dk + dk1, dv + dv1, dq + dq1)
            if masked:
                dk_ref[:, cols[0]] = dk
                dv_ref[:, cols[0]] = dv
            else:
                dk_ref[:, cols[0]] += dk
                dv_ref[:, cols[0]] += dv
            dq_ref[dq_rows, pl.ds(pl.multiple_of(dq_lane + 128 * pr, 128), 128)] += dq

    def small_ticks(i):
        for b in range(bits + 1):
            @pl.when(i == groups * (b + 1))
            def _(b=b):
                small_end(b)
                if b < bits:
                    small_start(b + 1)

    def key_block(kb, i):
        small_ticks(i)
        block(kb, kb, True, i)

        def other(qb, i):
            small_ticks(i)
            block(kb, qb, False, i)
            return i + groups
        i = lax.fori_loop(kb + 1, nb, other, i + groups)
        k_at = place(kb)
        dq_rows, dq_lane = dq_at(kb)
        for j, part in ((0, dq_ref[dq_rows, pl.ds(dq_lane, width)] * 0.125), (1, dk_ref[...]), (2, dv_ref[...])):
            low = part.astype(bf16)
            qkv_ref[pl.ds(k_at, blk), pl.ds(j * width, width)] = low
            if j != 1:
                hb_ref[j // 2] += jnp.sum(low.astype(f32), axis=0, keepdims=True)
        return i
    lax.fori_loop(0, nb, key_block, 0)
    for b in range(bits + 1):
        if groups * (b + 1) >= slots:
            small_end(b)
            if b < bits:
                small_start(b + 1)
    v, r = vb_ref[bits], rb_ref[bits]
    small_out[...] = v + jnp.concatenate([r[0:4], r[6:8], r[6:8]])

    tile = dim // 2

    def rest(i):
        return q_mid + i * (q_all - q_mid) // 10

    def head_grads(i, _):
        at = pl.ds(pl.multiple_of(i * tile, tile), tile)
        pulls = [fetch(src.at[:, at], g_ref.at[pl.ds(k * half, half)], 9 + k)
                 for k, src in enumerate((own_hbm, oth_hbm))]
        for pull in pulls:
            pull.wait()
        acc = (dot_tn(g_ref[pl.ds(0, half), :], qkv_ref[pl.ds(0, half), :])
               + dot_tn(g_ref[pl.ds(half, half), :], qkv_ref[pl.ds(half, half), :]))
        for j in range(3):
            part = acc[:, j * width:(j + 1) * width].reshape(tile // ch2, ch2, width).astype(bf16)
            t_ref[pl.ds((j * dim + i * tile) // ch2, tile // ch2)] = part
        ticks(rest(i), rest(i + 1))
        return 0
    lax.fori_loop(0, 2, head_grads, 0)
    x_copy.wait()
    for i in range(2):
        more = xrecv_ref[i].astype(f32).reshape(width // ch2, ch2, width)
        t_ref[mix_place(i)] = (t_ref[mix_place(i)].astype(f32) + more).astype(bf16)
    tcore_copy = remote(t_ref.at[pl.ds((1 - core) * n, n)], tmate_ref, tc_sem.at[0], tc_sem.at[1], mate)
    tcore_copy.start()
    lanes = width // 128

    def lane_view(ref, c, u):
        return ref.at[c, :, pl.ds(pl.multiple_of(u * 128, 128), 128)]
    trs_tick, trs_finish = ring_sum(
        n, lanes, pos, follow, lambda c, u: lane_view(t_ref, core * n + c, u), lambda c, u: lane_view(tmate_ref, c, u),
        lambda s, u: lane_view(tslot_ref, s, u), lambda u: lane_view(tfirst_ref, 0, u), ts_send, ts_recv)
    tag_tick, tag_finish = ring_spread(n, lanes, pos, core, follow, mate, lambda c, u: lane_view(tail_ref, c, u),
                                       ta_send, ta_recv, tm_send, tm_recv)

    def tail_ticks(lo, hi):
        def one(q, _):
            @pl.when(q < lanes * n)
            def _():
                trs_tick(q // lanes, lax.rem(q, lanes))

            @pl.when(q >= lanes * n)
            def _():
                @pl.when(q == lanes * n)
                def _():
                    tail_ref[core * n + lax.rem(pos + 1, n)] = tslot_ref[n - 2]
                r = q - lanes * n
                tag_tick(r // lanes, lax.rem(r, lanes))
            return 0
        lax.fori_loop(lo, hi, one, 0)

    for copy in w_copies:
        copy.wait()

    def da_copy(i):
        return remote(dsend_ref.at[i], drecv_ref.at[i], d_send.at[i], d_recv.at[i], peer)

    def send_rows(i, _):
        gq = qkv_ref[pl.ds(pl.multiple_of(half + i * piece, piece), piece), :]
        dsend_ref[i] = dot_nt(gq, w_ref[...]).astype(bf16)
        da_copy(i).start()
        ticks(rest(i + 2), rest(i + 3))
        return 0
    lax.fori_loop(0, 4, send_rows, 0)
    tcore_copy.wait()
    tail_ticks(0, lanes)

    def own_rows(i, _):
        at = pl.ds(pl.multiple_of(i * piece, piece), piece)
        da_ref[at, :] = dot_nt(qkv_ref[at, :], w_ref[...])
        tail_ticks(lanes + i, lanes + i + 1)
        ticks(rest(i + 6), rest(i + 7))
        return 0
    lax.fori_loop(0, 4, own_rows, 0)
    marks = [lanes + 4] + [lanes * n * m // 24 for m in (14, 24, 34)]
    ub_ref[0] = jnp.zeros((8, dim), f32)
    tok_copy.wait()

    def out_copy(i):
        at = pl.ds(pl.multiple_of(i * piece, piece), piece)
        return pltpu.make_async_copy(row_ref.at[at], gtok_hbm.at[at], o_sem.at[i])

    def first_norm(i, _):
        da_copy(i).wait()

        def norm_rows(j, _):
            to = pl.multiple_of(j * inner, inner)
            at = pl.ds(pl.multiple_of(i * piece + j * inner, inner), inner)
            x = row_ref[at, :].astype(f32)
            x = x - jnp.mean(x, axis=-1, keepdims=True)
            inv = lax.rsqrt(jnp.mean(x * x, axis=-1, keepdims=True) + EPSILON)
            h = x * inv
            e = da_ref[at, :] + drecv_ref[i, pl.ds(to, inner), :].astype(f32)
            eg = e * gain1_ref[...]
            back = inv * (eg - jnp.mean(eg, axis=-1, keepdims=True)
                          - h * jnp.mean(eg * h, axis=-1, keepdims=True))
            row_ref[at, :] = (gm_ref[at, :] + back).astype(bf16)
            ub_ref[0, 0:1, :] += jnp.sum(e * h, axis=0, keepdims=True)
            ub_ref[0, 1:2, :] += jnp.sum(e, axis=0, keepdims=True)
            return 0
        lax.fori_loop(0, 4, norm_rows, 0)
        out_copy(i).start()
        return 0
    for i in range(4):
        lax.fori_loop(i, i + 1, first_norm, 0)
        if i < 3:
            tail_ticks(marks[i], marks[i + 1])
    ub_ref[0, 2:3, pl.ds(0, width)] = hb_ref[0]
    ub_ref[0, 2:3, pl.ds(width, width)] = hb_ref[1]
    left = 2 * lanes * n - marks[3]
    for b in range(bits + 1):
        copy = small_copy(ub_ref, qb_ref, u_send, u_recv, b)
        copy.start()
        tail_ticks(marks[3] + b * left // (bits + 1), marks[3] + (b + 1) * left // (bits + 1))
        copy.wait()
        if b < bits:
            ub_ref[b + 1] = ub_ref[b] + qb_ref[b]
    v, r = ub_ref[bits], qb_ref[bits]
    last_out[...] = jnp.concatenate([v[0:2] + r[0:2], v[2:8]])
    for i in range(4):
        out_copy(i).wait()
    rs_finish()
    ag_finish()
    trs_finish()
    tag_finish()


def backward(size, count, qkv, att, att_recv, lse, gd, gu, a1, a1_other, w, mix, mix_other, small, tokens, gain1, gain2,
             cotangent, middle, grad_a2, blk=512):
    rows, total = qkv.shape
    width = total // 3
    half, dim = tokens.shape
    nb = rows // blk
    n = size // 2
    bits = size.bit_length() - 1
    hidden = gd.shape[1]
    gd, gu = (v.reshape(2, n, hidden // n, dim) for v in (gd, gu))
    ch, ch2 = hidden // n, 4 * dim // (2 * n)
    lanes = width // 128
    vm = pl.BlockSpec(memory_space=pltpu.VMEM)
    hb = pl.BlockSpec(memory_space=pl.ANY)
    sm = pl.BlockSpec(memory_space=pltpu.SMEM)
    V, S = pltpu.VMEM, pltpu.SemaphoreType.DMA
    q4 = half // 4
    return pl.pallas_call(
        functools.partial(backward_kernel, size, blk),
        in_specs=[sm, hb, vm, vm, vm, hb, hb, hb, hb, hb, vm, vm, vm, hb, vm, vm, hb, hb, hb],
        out_specs=[vm, vm, hb, vm, vm],
        out_shape=[jax.ShapeDtypeStruct((2 * n, ch, dim), bf16),
                   jax.ShapeDtypeStruct((2 * n, ch2, width), bf16),
                   jax.ShapeDtypeStruct((half, dim), bf16),
                   jax.ShapeDtypeStruct((8, dim), f32),
                   jax.ShapeDtypeStruct((8, dim), f32)],
        scratch_shapes=[
            V((rows, total), bf16), V((rows, width), bf16), V((nb, 8, blk), f32), V((half, 2 * width), f32),
            V((blk, width), f32), V((blk, width), f32), V((dim, total), bf16), V((half, dim), f32),
            V((4, q4, width), bf16), V((half, dim), bf16),
            V((2, n, ch, dim), bf16), V((2, n, ch, dim), bf16), V((n - 1, 2, ch, dim), bf16), V((2, ch, dim), bf16),
            V((ch, dim), bf16),
            V((2 * n, ch2, width), bf16), V((n, ch2, width), bf16), V((n - 1, ch2, width), bf16),
            V((1, ch2, width), bf16), V((2, width, width), bf16), V((2, width, width), bf16),
            V((half, dim), f32), V((4, q4, dim), bf16), V((4, q4, dim), bf16),
            V((bits + 1, 8, dim), f32), V((bits + 1, 8, dim), f32), V((bits + 1, 8, dim), f32),
            V((bits + 1, 8, dim), f32), V((2, 1, width), f32),
            S((11,)), S((2,)), S((2 * n - 2,)), S((2 * n - 2,)), S((2 * n - 2,)), S((2 * n - 2,)), S((2 * n,)),
            S((2 * n,)), S((2,)),
            S((2,)), S((lanes * (n - 1),)), S((lanes * (n - 1),)), S((lanes * (n - 1),)), S((lanes * (n - 1),)),
            S((lanes * n,)), S((lanes * n,)),
            S((4,)), S((4,)), S((bits + 1,)), S((bits + 1,)), S((bits + 1,)), S((bits + 1,)), S((4,)), S((4,)),
            S((2,)), S((4,))],
        compiler_params=pltpu.CompilerParams(collective_id=0, has_side_effects=True,
                                             vmem_limit_bytes=67_043_328),
        cost_estimate=pl.CostEstimate(flops=40_000_000_000, transcendentals=0, bytes_accessed=30_000_000),
        name="backward",
    )(count, qkv, att, att_recv, lse, gd, gu, a1, a1_other, w, mix, mix_other, small, tokens, gain1, gain2, cotangent,
      middle, grad_a2)


def mlp_kernel(a2_ref, gm_ref, mid_ref, up_ref, upo_ref, bias_ref, down_ref, downo_ref, dbias_ref,
               gd_ref, gu_ref, da2_ref, res_ref, small_ref,
               turn_ref, w_ref, v_ref, acc_ref):
    i = pl.program_id(0)
    steps = pl.num_programs(0)
    rows = a2_ref.shape[0]
    tile = w_ref.shape[1]

    @pl.when(i == 0)
    def _():
        turn_ref[...] = a2_ref[...].T
        da2_ref[...] = jnp.zeros_like(da2_ref)
        acc_ref[...] = jnp.zeros_like(acc_ref)
        small_ref[...] = jnp.zeros_like(small_ref)

    @pl.when(i < steps // 2)
    def _():
        w_ref[...] = up_ref[...]
        v_ref[...] = down_ref[...]

    @pl.when(i >= steps // 2)
    def _():
        w_ref[...] = upo_ref[...]
        v_ref[...] = downo_ref[...]
    half = rows // 2
    gd = gu = sums = None
    for r in range(2):
        at = pl.ds(r * half, half)
        gm = gm_ref[at, :]
        pre = dot32(a2_ref[at, :], w_ref[...]) + bias_ref[0]
        grad = dot_nt(gm, v_ref[...])
        act, slope = gelu_pair(pre)
        act = act.astype(bf16)
        grad = (grad * slope).astype(bf16)
        acc_ref[at, :] += dot32(act, v_ref[...])
        da2_ref[at, :] += dot_nt(grad, w_ref[...])
        gd1 = dot_tn(act, gm)
        gu1 = dot32(turn_ref[:, r * half:(r + 1) * half], grad)
        s1 = jnp.sum(grad.astype(f32), axis=0, keepdims=True)
        gd, gu, sums = (gd1, gu1, s1) if r == 0 else (gd + gd1, gu + gu1, sums + s1)
    gd_ref[0] = gd.astype(bf16)
    gu_ref[0] = gu.astype(bf16)
    small_ref[pl.ds(4 + i // 2, 1), pl.ds(pl.multiple_of(lax.rem(i, 2) * tile, 128), tile)] = sums

    @pl.when(i == steps - 1)
    def _():
        res_ref[...] = (mid_ref[...] + BRANCH * (acc_ref[...] + dbias_ref[...])).astype(bf16)


def mlp(a2, grad_mlp, middle, up, up_other, bias, bias_other, down, down_other, down_bias):
    rows, dim = a2.shape
    hidden = up.shape[1]
    tile = dim // 2
    per = hidden // tile
    bias = jnp.concatenate([bias, bias_other]).reshape(2 * per, 1, tile)
    whole = pl.BlockSpec((rows, dim), lambda i: (0, 0), pipeline_mode=pl.Buffered(1))
    first = lambda i: jnp.minimum(i, per - 1)
    later = lambda i: jnp.maximum(i - per, 0)
    return pl.pallas_call(
        mlp_kernel,
        grid=(2 * per,),
        in_specs=[whole, whole, whole,
                  pl.BlockSpec((dim, tile), lambda i: (0, first(i))),
                  pl.BlockSpec((dim, tile), lambda i: (0, later(i))),
                  pl.BlockSpec((1, 1, tile), lambda i: (i, 0, 0)),
                  pl.BlockSpec((tile, dim), lambda i: (first(i), 0)),
                  pl.BlockSpec((tile, dim), lambda i: (later(i), 0)),
                  pl.BlockSpec((1, dim), lambda i: (0, 0))],
        out_specs=[pl.BlockSpec((1, tile, dim), lambda i: (i // per, i % per, 0)),
                   pl.BlockSpec((1, dim, tile), lambda i: (i // per, i % per // 2, i % 2)),
                   pl.BlockSpec((rows, dim), lambda i: (0, 0)),
                   pl.BlockSpec((rows, dim), lambda i: (0, 0)),
                   pl.BlockSpec((8, dim), lambda i: (0, 0))],
        out_shape=[jax.ShapeDtypeStruct((2, hidden, dim), bf16),
                   jax.ShapeDtypeStruct((2, hidden, dim), bf16),
                   jax.ShapeDtypeStruct((rows, dim), f32),
                   jax.ShapeDtypeStruct((rows, dim), bf16),
                   jax.ShapeDtypeStruct((8, dim), f32)],
        scratch_shapes=[pltpu.VMEM((dim, rows), bf16), pltpu.VMEM((dim, tile), bf16), pltpu.VMEM((tile, dim), bf16),
                        pltpu.VMEM((rows, dim), f32)],
        compiler_params=pltpu.CompilerParams(vmem_limit_bytes=60 << 20),
        cost_estimate=pl.CostEstimate(flops=29_000_000_000, transcendentals=0, bytes_accessed=30_000_000),
        name="mlp",
    )(a2, grad_mlp, middle, up, up_other, bias, down, down_other, down_bias[None])


def to_peer(v):
    return lax.ppermute(v, "tensor", SWAP)


def row_stats(v):
    centre = jnp.mean(v, axis=-1, keepdims=True)
    centred = v - centre
    inv = lax.rsqrt(jnp.mean(centred * centred, axis=-1, keepdims=True) + EPSILON)
    return centre, inv


def dot32(a, b):
    return jnp.dot(a, b, preferred_element_type=f32)


def dot_nt(a, b):
    return lax.dot_general(a, b, NT, preferred_element_type=f32)


def dot_tn(a, b):
    return lax.dot_general(a, b, TN, preferred_element_type=f32)


def xor_step(v, size, bit):
    return lax.ppermute(v, "dp", [(i, i ^ (1 << bit)) for i in range(size)])


def gelu_pair(v):
    t = jnp.tanh(GELU_C * (v + 0.044715 * v * v * v))
    return 0.5 * v * (1.0 + t), 0.5 * (1.0 + t) + 0.5 * v * (1.0 - t * t) * (
        GELU_C * (1.0 + 3.0 * 0.044715 * v * v))


def local(
    tokens,
    seq_count,
    first_gain,
    first_shift,
    heads_weight,
    heads_bias,
    mixing_weight,
    mixing_bias,
    second_gain,
    second_shift,
    up_weight,
    up_bias,
    down_weight,
    down_bias,
    cotangent,
):
    size = lax.axis_size("dp")
    me = lax.axis_index("dp")
    side = lax.axis_index("tensor")
    info = jnp.stack([side.astype(jnp.int32), seq_count[0]])
    half, dim = tokens.shape
    width = heads_weight.shape[2]
    hidden = up_weight.shape[1]

    pu, pd, pm = dim // size, hidden // size, width // size
    piece = jnp.concatenate([
        lax.dynamic_slice(up_weight, (me * pu, 0), (pu, hidden // 2)),
        lax.dynamic_slice(up_weight, (me * pu, hidden // 2), (pu, hidden // 2)),
        lax.dynamic_slice_in_dim(down_weight, me * pd, pd, 0),
        lax.dynamic_slice_in_dim(mixing_weight, me * pm, pm, 0)])
    piece = to_peer(piece)
    up_bias_other = to_peer(up_bias)

    x = tokens.astype(f32)
    centre1, inv1 = row_stats(x)
    a1 = ((x - centre1) * inv1 * first_gain + first_shift).astype(bf16)
    piece, a1 = lax.optimization_barrier((piece, a1))
    a1_other = to_peer(a1)
    packed = lax.all_gather(piece, "dp", axis=0)
    up_other = jnp.concatenate([packed[:, :pu].reshape(dim, hidden // 2),
                                packed[:, pu:2 * pu].reshape(dim, hidden // 2)], axis=1)
    down_other = packed[:, 2 * pu:2 * pu + pd].reshape(hidden, dim)
    mix_other = packed[:, 2 * pu + pd:].reshape(width, dim)
    bias3 = jnp.stack([heads_bias[0], jnp.zeros_like(heads_bias[0]), heads_bias[1]])
    qkv, att, lse = attn_forward(info, a1, a1_other, heads_weight, bias3)
    att_mine = att[:half]
    att_recv = to_peer(att[half:])
    middle = x + BRANCH * (dot32(att_mine, mixing_weight) + dot32(att_recv, mix_other) + mixing_bias)
    centre2, inv2 = row_stats(middle)
    h2 = (middle - centre2) * inv2
    a2 = (h2 * second_gain + second_shift).astype(bf16)

    grad_mlp = (BRANCH * cotangent.astype(f32)).astype(bf16)
    gd, gu, grad_a2, result, small = mlp(a2, grad_mlp, middle, up_weight, up_other, up_bias, up_bias_other,
                                         down_weight, down_other, down_bias)
    fin, tail, grad_tokens, small, last = backward(
        size, seq_count, qkv, att, att_recv, lse, gd, gu, a1, a1_other, heads_weight, mixing_weight, mix_other, small,
        tokens, first_gain[None], second_gain[None], cotangent, middle, grad_a2)
    groups = 1.0 / size
    small = small * groups
    last = last * groups
    fin = fin.reshape(2, hidden, dim).astype(f32) * groups
    tail = tail.reshape(4 * dim, width).astype(f32) * groups
    grad_up = fin[1]
    return (
        result,
        grad_tokens,
        last[0],
        last[1],
        tail[:3 * dim].reshape(3, dim, width),
        last[2].reshape(2, width),
        jnp.concatenate([tail[3 * dim:3 * dim + width], tail[3 * dim + width:]], axis=1),
        small[3],
        small[1],
        small[2],
        jnp.concatenate([grad_up[:dim], grad_up[dim:]], axis=1),
        small[4:6].reshape(hidden),
        fin[0],
        small[0],
    )


def solution(mesh):
    placed = (
        P(("dp", "tensor"), None),
        P("dp"),
        P(),
        P(),
        P(None, None, "tensor"),
        P(None, "tensor"),
        P("tensor", None),
        P(),
        P(),
        P(),
        P(None, "tensor"),
        P("tensor"),
        P("tensor", None),
        P(),
        P(("dp", "tensor"), None),
    )
    return jax.shard_map(
        local,
        mesh=mesh,
        in_specs=placed,
        out_specs=(
            P(("dp", "tensor"), None),
            P(("dp", "tensor"), None),
            P(),
            P(),
            P(None, None, "tensor"),
            P(None, "tensor"),
            P("tensor", None),
            P(),
            P(),
            P(),
            P(None, "tensor"),
            P("tensor"),
            P("tensor", None),
            P(),
        ),
        check_vma=False,
    )
```

```python
import functools, math
import jax
import jax.numpy as jnp
from jax import lax
from jax.experimental import pallas as pl
from jax.experimental.pallas import tpu as pltpu
from jax.sharding import PartitionSpec as P

HEAD = 64
DEPTH = 12
EPSILON = 1e-05
BRANCH = 1.0 / math.sqrt(DEPTH)
GELU_C = math.sqrt(2.0 / math.pi)
LOG2E = math.log2(math.e)
NT = (((1,), (1,)), ((), ()))
TN = (((0,), (0,)), ((), ()))
f32 = jnp.float32
bf16 = jnp.bfloat16


def remote(src, dst, send, recv, where):
    return pltpu.make_async_remote_copy(src_ref=src, dst_ref=dst, send_sem=send, recv_sem=recv,
                                        device_id=where, device_id_type=pl.DeviceIdType.MESH)


def ring_sum(n, lanes, pos, where, local, mate, slot, first, send, recv):
    def hop(src, s, u):
        return remote(src, slot(s, u), send.at[s * lanes + u], recv.at[s * lanes + u], where)

    def at(c):
        return lax.rem(c + 2 * n, n)

    def tick(k, u):
        @pl.when(k == 0)
        def _():
            c = at(pos)
            first(u)[...] = (local(c, u)[...].astype(f32) + mate(c, u)[...].astype(f32)).astype(bf16)
            hop(first(u), 0, u).start()

        @pl.when(k > 0)
        def _():
            c = at(pos - k)
            here = slot(k - 1, u)
            hop(here, k - 1, u).wait_recv()
            here[...] = (here[...].astype(f32) + local(c, u)[...].astype(f32)
                         + mate(c, u)[...].astype(f32)).astype(bf16)

            @pl.when(k < n - 1)
            def _():
                hop(here, k, u).start()

    def finish():
        def one(s, _):
            for u in range(lanes):
                hop(slot(s, u), s, u).wait_send()
            return 0
        lax.fori_loop(0, n - 1, one, 0)
    return tick, finish


def ring_spread(n, lanes, pos, core, where, mate, view, send, recv, m_send, m_recv):
    def spot(c):
        return core * n + lax.rem(c + 2 * n, n)

    def hop(s, u):
        chunk = view(spot(pos + 1 - s), u)
        return remote(chunk, chunk, send.at[s * lanes + u], recv.at[s * lanes + u], where)

    def over(s, u):
        chunk = view(spot(pos + 1 - s), u)
        return remote(chunk, chunk, m_send.at[s * lanes + u], m_recv.at[s * lanes + u], mate)

    def tick(k, u):
        @pl.when(k > 0)
        def _():
            hop(k - 1, u).wait_recv()

        @pl.when(k < n - 1)
        def _():
            hop(k, u).start()
        over(k, u).start()

    def finish():
        def one(s, _):
            for u in range(lanes):
                @pl.when(s < n - 1)
                def _():
                    hop(s, u).wait_send()
                over(s, u).wait()
            return 0
        lax.fori_loop(0, n, one, 0)
    return tick, finish


def backward_kernel(size, blk, count_ref, qkv_hbm, att_ref, arecv_ref, lse_ref, gd_hbm, gu_hbm, own_hbm, oth_hbm,
                    w_hbm, mix_ref, mixo_ref, small_ref, tok_hbm, gain1_ref, gain2_ref, cot_hbm, mid_hbm, da2_hbm,
                    fin_ref, tail_ref, gtok_hbm, small_out, last_out,
                    qkv_ref, g_ref, delta_ref, dq_ref, dk_ref, dv_ref, w_ref, gm_ref, gsend_ref, row_ref,
                    gl_ref, mate_ref, slot_ref, first_ref, yin_ref,
                    t_ref, tmate_ref, tslot_ref, tfirst_ref, xsend_ref, xrecv_ref,
                    da_ref, dsend_ref, drecv_ref, vb_ref, rb_ref, ub_ref, qb_ref, hb_ref,
                    in_sem, c_sem, s_send, s_recv, a_send, a_recv, m_send, m_recv, y_sem,
                    tc_sem, ts_send, ts_recv, ta_send, ta_recv, tm_send, tm_recv,
                    d_send, d_recv, v_send, v_recv, u_send, u_recv, g_send, g_recv, x_sem, o_sem):
    n = size // 2
    bits = size.bit_length() - 1
    rows, total = qkv_ref.shape
    half = rows // 2
    width = total // 3
    dim = w_hbm.shape[1]
    nb = rows // blk
    me, side = lax.axis_index("dp"), lax.axis_index("tensor")
    core, chip = lax.rem(me, 2), me // 2
    odd = lax.rem(chip, 2)
    p = (1 - odd) * (chip // 2) + odd * (n - 1 - chip // 2)

    def chip_at(q):
        up = q // (n // 2)
        return (1 - up) * 2 * q + up * (2 * (n - 1 - q) + 1)
    pos = (1 - core) * p + core * lax.rem(n - p, n)
    step = 1 - 2 * core
    follow = {"dp": 2 * chip_at(lax.rem(p + step + n, n)) + core}
    before = {"dp": 2 * chip_at(lax.rem(p - step + n, n)) + core}
    mate = {"dp": me + 1 - 2 * core}
    peer = {"tensor": 1 - side}
    partner = [mate] + [{"dp": me + (1 - 2 * lax.rem(me // (1 << b), 2)) * (1 << b)} for b in range(1, bits)] + [peer]

    def fetch(src, dst, i):
        copy = pltpu.make_async_copy(src, dst, in_sem.at[i])
        copy.start()
        return copy
    da2_copy = fetch(da2_hbm, da_ref, 0)
    mid_copy = fetch(mid_hbm, dq_ref, 1)
    cot_copy = fetch(cot_hbm, row_ref, 7)
    gl_copies = [pltpu.make_async_copy(src, gl_ref, in_sem.at[2]) for src in (gd_hbm, gu_hbm)]
    for which in range(2):
        pl.when(core == which)(gl_copies[which].start)
    q_copy = fetch(qkv_hbm, qkv_ref, 3)
    w_copies = [fetch(w_hbm.at[j], w_ref.at[:, pl.ds(j * width, width)], 4 + j) for j in range(3)]
    ch2 = t_ref.shape[1]

    barrier = pltpu.get_barrier_semaphore()
    friends = [follow, before] + partner
    for to in friends:
        pl.semaphore_signal(barrier, inc=1, device_id=to, device_id_type=pl.DeviceIdType.MESH)
    pl.semaphore_wait(barrier, len(friends))

    core_copies = [remote(src, mate_ref, c_sem.at[0], c_sem.at[1], mate) for src in (gu_hbm, gd_hbm)]
    for which in range(2):
        pl.when(core == which)(core_copies[which].start)

    rs_tick, rs_finish = ring_sum(
        n, 2, pos, follow, lambda c, u: gl_ref.at[1 - u, c], lambda c, u: mate_ref.at[1 - u, c],
        lambda s, u: slot_ref.at[s, 1 - u], lambda u: first_ref.at[1 - u], s_send, s_recv)
    cut = dim // 2

    def fin_view(c, u):
        return fin_ref.at[c, :, pl.ds(pl.multiple_of(u * cut, 128), cut)]
    ag_tick, ag_finish = ring_spread(n, 2, pos, core, follow, mate, fin_view, a_send, a_recv, m_send, m_recv)
    y_copy = remote(slot_ref.at[n - 2, 1], yin_ref, y_sem.at[0], y_sem.at[1], peer)

    def tick(q):
        @pl.when(q == 0)
        def _():
            gl_copies[0].wait()
            core_copies[0].wait()

        @pl.when(q < 2 * n)
        def _():
            rs_tick(q // 2, lax.rem(q, 2))

            @pl.when(q == 2 * n - 2)
            def _():
                y_copy.start()

        @pl.when(q == 2 * n)
        def _():
            y_copy.wait()
            fin_ref[core * n + lax.rem(pos + 1, n)] = (slot_ref[n - 2, 0].astype(f32)
                                                       + yin_ref[...].astype(f32)).astype(bf16)

        @pl.when(q > 2 * n)
        def _():
            r = q - 2 * n - 1
            ag_tick(r // 2, lax.rem(r, 2))
    q_rs, q_all = 2 * n + 1, 4 * n + 1

    def ticks(lo, hi):
        def one(k, _):
            tick(k)
            return 0
        lax.fori_loop(lo, hi, one, 0)

    piece = half // 4
    vb_ref[0] = small_ref[...]
    da2_copy.wait()
    mid_copy.wait()
    cot_copy.wait()
    inner = piece // 4

    def g_copy(i):
        return remote(gsend_ref.at[i], g_ref.at[pl.ds(pl.multiple_of(half + i * piece, piece), piece)],
                      g_send.at[i], g_recv.at[i], peer)

    def second_norm(i, _):
        def norm_rows(j, _):
            to = pl.multiple_of(j * inner, inner)
            at = pl.ds(pl.multiple_of(i * piece + j * inner, inner), inner)
            x = dq_ref[at, :]
            x = x - jnp.mean(x, axis=-1, keepdims=True)
            inv = lax.rsqrt(jnp.mean(x * x, axis=-1, keepdims=True) + EPSILON)
            h = x * inv
            e = da_ref[at, :]
            eg = e * gain2_ref[...]
            g_out = row_ref[at, :].astype(f32)
            gm = g_out + inv * (eg - jnp.mean(eg, axis=-1, keepdims=True)
                                - h * jnp.mean(eg * h, axis=-1, keepdims=True))
            gm_ref[at, :] = gm
            dsend_ref[i, pl.ds(to, inner), :] = (BRANCH * gm).astype(bf16)
            vb_ref[0, 0:1, :] += BRANCH * jnp.sum(g_out, axis=0, keepdims=True)
            vb_ref[0, 1:2, :] += jnp.sum(e * h, axis=0, keepdims=True)
            vb_ref[0, 2:3, :] += jnp.sum(e, axis=0, keepdims=True)
            vb_ref[0, 3:4, :] += BRANCH * jnp.sum(gm, axis=0, keepdims=True)
            return 0
        lax.fori_loop(0, 4, norm_rows, 0)
        ga = dsend_ref[i]
        gsend_ref[i] = dot_nt(ga, mixo_ref[...]).astype(bf16)
        g_copy(i).start()
        return 0
    lax.fori_loop(0, 4, second_norm, 0)
    tok_copy = fetch(tok_hbm, row_ref, 8)

    def small_copy(buf, inbox, send, recv, b):
        return remote(buf.at[b], inbox.at[b], send.at[b], recv.at[b], partner[b])

    def small_start(b):
        small_copy(vb_ref, rb_ref, v_send, v_recv, b).start()

    def small_end(b):
        small_copy(vb_ref, rb_ref, v_send, v_recv, b).wait()
        if b < bits:
            vb_ref[b + 1] = vb_ref[b] + rb_ref[b]
    small_start(0)

    pre = 6 * n // 8
    ticks(0, pre // 3)
    for i in range(4):
        g_ref[pl.ds(i * piece, piece), :] = dot_nt(dsend_ref[i], mix_ref[...]).astype(bf16)

    def mix_grad(lhs_ref):
        acc = jnp.zeros((width, dim), f32)
        for i in range(4):
            acc += dot_tn(lhs_ref[pl.ds(i * piece, piece), :], dsend_ref[i])
        return acc
    first_mix = 3 * dim // ch2
    acc = mix_grad(arecv_ref)
    for i in range(2):
        xsend_ref[i] = acc[:, i * width:(i + 1) * width].astype(bf16)
    x_copy = remote(xsend_ref, xrecv_ref, x_sem.at[0], x_sem.at[1], peer)
    ticks(pre // 3, 2 * pre // 3)
    acc = mix_grad(att_ref)

    def mix_place(i):
        return pl.ds(first_mix + i * (width // ch2), width // ch2)
    for i in range(2):
        t_ref[mix_place(i)] = acc[:, i * width:(i + 1) * width].reshape(width // ch2, ch2, width).astype(bf16)
    hb_ref[...] = jnp.zeros_like(hb_ref)
    dq_ref[...] = jnp.zeros_like(dq_ref)
    q_copy.wait()
    ticks(2 * pre // 3, pre)
    for i in range(4):
        g_copy(i).wait()
    x_copy.start()

    def local_block(b):
        return lax.rem(b + side * (nb // 2), nb)

    def place(b):
        return pl.multiple_of(local_block(b) * blk, blk)

    def dq_at(b):
        spot = local_block(b)
        return (pl.ds(pl.multiple_of(lax.rem(spot, nb // 2) * blk, blk), blk),
                pl.multiple_of(spot // (nb // 2) * width, 128))
    pick = (lax.broadcasted_iota(jnp.int32, (8, width), 1) // HEAD
            == lax.broadcasted_iota(jnp.int32, (8, width), 0)).astype(bf16)

    def deltas(b, _):
        at = pl.ds(place(b), blk)
        prod = g_ref[at, :].astype(f32) * att_ref[at, :].astype(f32)
        high = prod.astype(bf16)
        low = (prod - high.astype(f32)).astype(bf16)
        delta_ref[b] = dot_nt(pick, high) + dot_nt(pick, low)
        return 0
    lax.fori_loop(0, nb, deltas, 0)

    lane_lo = lax.broadcasted_iota(jnp.int32, (blk, 128), 1) < HEAD
    count = count_ref[0]
    groups = width // 128
    slots = groups * nb * (nb + 1) // 2
    slow = 11 * slots // 15
    q_mid = q_rs + (q_all - q_rs) // 2

    def tick_mark(i):
        early = pre + i * (q_rs - pre) // slow
        late = q_rs + (i - slow) * (q_mid - q_rs) // (slots - slow)
        return jnp.where(i < slow, early, late)

    def block(kb, qb, masked, i):
        k_at, q_at = place(kb), place(qb)
        dq_rows, dq_lane = dq_at(qb)
        if masked:
            keep = (lax.broadcasted_iota(jnp.int32, (blk, blk), 0)
                    <= lax.broadcasted_iota(jnp.int32, (blk, blk), 1))
        else:
            apart = jnp.where(kb * count // nb == qb * count // nb, 0.0, 1e30)
        for pr in range(groups):
            ticks(tick_mark(i + pr), tick_mark(i + pr + 1))
            cols = [pl.ds(j * width + 128 * pr, 128) for j in range(3)]
            q = qkv_ref[pl.ds(q_at, blk), cols[0]]
            g = g_ref[pl.ds(q_at, blk), cols[0]]
            k = qkv_ref[pl.ds(k_at, blk), cols[1]]
            v = qkv_ref[pl.ds(k_at, blk), cols[2]]
            dk = dv = dq = None
            for h in range(2):
                mine = lane_lo if h == 0 else ~lane_lo
                head = 2 * pr + h
                kh = jnp.where(mine, k, bf16(0))
                vh = jnp.where(mine, v, bf16(0))
                s = dot_nt(kh, q) * LOG2E
                lse = lse_ref[qb, pl.ds(head, 1), :]
                if not masked:
                    lse = lse + apart
                e = jnp.exp2(s - lse)
                if masked:
                    e = jnp.where(keep, e, 0.0)
                dp = dot_nt(vh, g)
                ds = (e * (dp - delta_ref[qb, pl.ds(head, 1), :])).astype(bf16)
                e = e.astype(bf16)
                dv1 = dot32(e, jnp.where(mine, g, bf16(0)))
                dk1 = dot32(ds, jnp.where(mine, q, bf16(0)))
                dq1 = dot_tn(ds, kh)
                dk, dv, dq = (dk1, dv1, dq1) if h == 0 else (dk + dk1, dv + dv1, dq + dq1)
            if masked:
                dk_ref[:, cols[0]] = dk
                dv_ref[:, cols[0]] = dv
            else:
                dk_ref[:, cols[0]] += dk
                dv_ref[:, cols[0]] += dv
            dq_ref[dq_rows, pl.ds(pl.multiple_of(dq_lane + 128 * pr, 128), 128)] += dq

    def small_ticks(i):
        for b in range(bits + 1):
            @pl.when(i == groups * (b + 1))
            def _(b=b):
                small_end(b)
                if b < bits:
                    small_start(b + 1)

    def key_block(kb, i):
        small_ticks(i)
        block(kb, kb, True, i)

        def other(qb, i):
            small_ticks(i)
            block(kb, qb, False, i)
            return i + groups
        i = lax.fori_loop(kb + 1, nb, other, i + groups)
        k_at = place(kb)
        dq_rows, dq_lane = dq_at(kb)
        for j, part in ((0, dq_ref[dq_rows, pl.ds(dq_lane, width)] * 0.125), (1, dk_ref[...]), (2, dv_ref[...])):
            low = part.astype(bf16)
            qkv_ref[pl.ds(k_at, blk), pl.ds(j * width, width)] = low
            if j != 1:
                hb_ref[j // 2] += jnp.sum(low.astype(f32), axis=0, keepdims=True)
        return i
    lax.fori_loop(0, nb, key_block, 0)
    for b in range(bits + 1):
        if groups * (b + 1) >= slots:
            small_end(b)
            if b < bits:
                small_start(b + 1)
    v, r = vb_ref[bits], rb_ref[bits]
    small_out[...] = v + jnp.concatenate([r[0:4], r[6:8], r[6:8]])

    tile = dim // 2

    def rest(i):
        return q_mid + i * (q_all - q_mid) // 10

    def head_grads(i, _):
        at = pl.ds(pl.multiple_of(i * tile, tile), tile)
        pulls = [fetch(src.at[:, at], g_ref.at[pl.ds(k * half, half)], 9 + k)
                 for k, src in enumerate((own_hbm, oth_hbm))]
        for pull in pulls:
            pull.wait()
        acc = (dot_tn(g_ref[pl.ds(0, half), :], qkv_ref[pl.ds(0, half), :])
               + dot_tn(g_ref[pl.ds(half, half), :], qkv_ref[pl.ds(half, half), :]))
        for j in range(3):
            part = acc[:, j * width:(j + 1) * width].reshape(tile // ch2, ch2, width).astype(bf16)
            t_ref[pl.ds((j * dim + i * tile) // ch2, tile // ch2)] = part
        ticks(rest(i), rest(i + 1))
        return 0
    lax.fori_loop(0, 2, head_grads, 0)
    x_copy.wait()
    for i in range(2):
        more = xrecv_ref[i].astype(f32).reshape(width // ch2, ch2, width)
        t_ref[mix_place(i)] = (t_ref[mix_place(i)].astype(f32) + more).astype(bf16)
    tcore_copy = remote(t_ref.at[pl.ds((1 - core) * n, n)], tmate_ref, tc_sem.at[0], tc_sem.at[1], mate)
    tcore_copy.start()
    lanes = width // 128

    def lane_view(ref, c, u):
        return ref.at[c, :, pl.ds(pl.multiple_of(u * 128, 128), 128)]
    trs_tick, trs_finish = ring_sum(
        n, lanes, pos, follow, lambda c, u: lane_view(t_ref, core * n + c, u), lambda c, u: lane_view(tmate_ref, c, u),
        lambda s, u: lane_view(tslot_ref, s, u), lambda u: lane_view(tfirst_ref, 0, u), ts_send, ts_recv)
    tag_tick, tag_finish = ring_spread(n, lanes, pos, core, follow, mate, lambda c, u: lane_view(tail_ref, c, u),
                                       ta_send, ta_recv, tm_send, tm_recv)

    def tail_ticks(lo, hi):
        def one(q, _):
            @pl.when(q < lanes * n)
            def _():
                trs_tick(q // lanes, lax.rem(q, lanes))

            @pl.when(q >= lanes * n)
            def _():
                @pl.when(q == lanes * n)
                def _():
                    tail_ref[core * n + lax.rem(pos + 1, n)] = tslot_ref[n - 2]
                r = q - lanes * n
                tag_tick(r // lanes, lax.rem(r, lanes))
            return 0
        lax.fori_loop(lo, hi, one, 0)

    for copy in w_copies:
        copy.wait()

    def da_copy(i):
        return remote(dsend_ref.at[i], drecv_ref.at[i], d_send.at[i], d_recv.at[i], peer)

    def send_rows(i, _):
        gq = qkv_ref[pl.ds(pl.multiple_of(half + i * piece, piece), piece), :]
        dsend_ref[i] = dot_nt(gq, w_ref[...]).astype(bf16)
        da_copy(i).start()
        ticks(rest(i + 2), rest(i + 3))
        return 0
    lax.fori_loop(0, 4, send_rows, 0)
    tcore_copy.wait()
    tail_ticks(0, lanes)

    def own_rows(i, _):
        at = pl.ds(pl.multiple_of(i * piece, piece), piece)
        da_ref[at, :] = dot_nt(qkv_ref[at, :], w_ref[...])
        tail_ticks(lanes + i, lanes + i + 1)
        ticks(rest(i + 6), rest(i + 7))
        return 0
    lax.fori_loop(0, 4, own_rows, 0)
    marks = [lanes + 4] + [lanes * n * m // 24 for m in (14, 24, 34)]
    ub_ref[0] = jnp.zeros((8, dim), f32)
    tok_copy.wait()

    def out_copy(i):
        at = pl.ds(pl.multiple_of(i * piece, piece), piece)
        return pltpu.make_async_copy(row_ref.at[at], gtok_hbm.at[at], o_sem.at[i])

    def first_norm(i, _):
        da_copy(i).wait()

        def norm_rows(j, _):
            to = pl.multiple_of(j * inner, inner)
            at = pl.ds(pl.multiple_of(i * piece + j * inner, inner), inner)
            x = row_ref[at, :].astype(f32)
            x = x - jnp.mean(x, axis=-1, keepdims=True)
            inv = lax.rsqrt(jnp.mean(x * x, axis=-1, keepdims=True) + EPSILON)
            h = x * inv
            e = da_ref[at, :] + drecv_ref[i, pl.ds(to, inner), :].astype(f32)
            eg = e * gain1_ref[...]
            back = inv * (eg - jnp.mean(eg, axis=-1, keepdims=True)
                          - h * jnp.mean(eg * h, axis=-1, keepdims=True))
            row_ref[at, :] = (gm_ref[at, :] + back).astype(bf16)
            ub_ref[0, 0:1, :] += jnp.sum(e * h, axis=0, keepdims=True)
            ub_ref[0, 1:2, :] += jnp.sum(e, axis=0, keepdims=True)
            return 0
        lax.fori_loop(0, 4, norm_rows, 0)
        out_copy(i).start()
        return 0
    for i in range(4):
        lax.fori_loop(i, i + 1, first_norm, 0)
        if i < 3:
            tail_ticks(marks[i], marks[i + 1])
    ub_ref[0, 2:3, pl.ds(0, width)] = hb_ref[0]
    ub_ref[0, 2:3, pl.ds(width, width)] = hb_ref[1]
    left = 2 * lanes * n - marks[3]
    for b in range(bits + 1):
        copy = small_copy(ub_ref, qb_ref, u_send, u_recv, b)
        copy.start()
        tail_ticks(marks[3] + b * left // (bits + 1), marks[3] + (b + 1) * left // (bits + 1))
        copy.wait()
        if b < bits:
            ub_ref[b + 1] = ub_ref[b] + qb_ref[b]
    v, r = ub_ref[bits], qb_ref[bits]
    last_out[...] = jnp.concatenate([v[0:2] + r[0:2], v[2:8]])
    for i in range(4):
        out_copy(i).wait()
    rs_finish()
    ag_finish()
    trs_finish()
    tag_finish()


def backward(size, count, qkv, att, att_recv, lse, gd, gu, a1, a1_other, w, mix, mix_other, small, tokens, gain1, gain2,
             cotangent, middle, grad_a2, blk=512):
    rows, total = qkv.shape
    width = total // 3
    half, dim = tokens.shape
    nb = rows // blk
    n = size // 2
    bits = size.bit_length() - 1
    hidden = gd.shape[1]
    gd, gu = (v.reshape(2, n, hidden // n, dim) for v in (gd, gu))
    ch, ch2 = hidden // n, 4 * dim // (2 * n)
    lanes = width // 128
    vm = pl.BlockSpec(memory_space=pltpu.VMEM)
    hb = pl.BlockSpec(memory_space=pl.ANY)
    sm = pl.BlockSpec(memory_space=pltpu.SMEM)
    V, S = pltpu.VMEM, pltpu.SemaphoreType.DMA
    q4 = half // 4
    return pl.pallas_call(
        functools.partial(backward_kernel, size, blk),
        in_specs=[sm, hb, vm, vm, vm, hb, hb, hb, hb, hb, vm, vm, vm, hb, vm, vm, hb, hb, hb],
        out_specs=[vm, vm, hb, vm, vm],
        out_shape=[jax.ShapeDtypeStruct((2 * n, ch, dim), bf16),
                   jax.ShapeDtypeStruct((2 * n, ch2, width), bf16),
                   jax.ShapeDtypeStruct((half, dim), bf16),
                   jax.ShapeDtypeStruct((8, dim), f32),
                   jax.ShapeDtypeStruct((8, dim), f32)],
        scratch_shapes=[
            V((rows, total), bf16), V((rows, width), bf16), V((nb, 8, blk), f32), V((half, 2 * width), f32),
            V((blk, width), f32), V((blk, width), f32), V((dim, total), bf16), V((half, dim), f32),
            V((4, q4, width), bf16), V((half, dim), bf16),
            V((2, n, ch, dim), bf16), V((2, n, ch, dim), bf16), V((n - 1, 2, ch, dim), bf16), V((2, ch, dim), bf16),
            V((ch, dim), bf16),
            V((2 * n, ch2, width), bf16), V((n, ch2, width), bf16), V((n - 1, ch2, width), bf16),
            V((1, ch2, width), bf16), V((2, width, width), bf16), V((2, width, width), bf16),
            V((half, dim), f32), V((4, q4, dim), bf16), V((4, q4, dim), bf16),
            V((bits + 1, 8, dim), f32), V((bits + 1, 8, dim), f32), V((bits + 1, 8, dim), f32),
            V((bits + 1, 8, dim), f32), V((2, 1, width), f32),
            S((11,)), S((2,)), S((2 * n - 2,)), S((2 * n - 2,)), S((2 * n - 2,)), S((2 * n - 2,)), S((2 * n,)),
            S((2 * n,)), S((2,)),
            S((2,)), S((lanes * (n - 1),)), S((lanes * (n - 1),)), S((lanes * (n - 1),)), S((lanes * (n - 1),)),
            S((lanes * n,)), S((lanes * n,)),
            S((4,)), S((4,)), S((bits + 1,)), S((bits + 1,)), S((bits + 1,)), S((bits + 1,)), S((4,)), S((4,)),
            S((2,)), S((4,))],
        compiler_params=pltpu.CompilerParams(collective_id=0, has_side_effects=True,
                                             vmem_limit_bytes=67_043_328),
        cost_estimate=pl.CostEstimate(flops=40_000_000_000, transcendentals=0, bytes_accessed=30_000_000),
        name="backward",
    )(count, qkv, att, att_recv, lse, gd, gu, a1, a1_other, w, mix, mix_other, small, tokens, gain1, gain2, cotangent,
      middle, grad_a2)


def ring_place(size):
    n = size // 2
    me, side = lax.axis_index("dp"), lax.axis_index("tensor")
    core, chip = lax.rem(me, 2), me // 2
    odd = lax.rem(chip, 2)
    p = (1 - odd) * (chip // 2) + odd * (n - 1 - chip // 2)

    def chip_at(q):
        up = q // (n // 2)
        return (1 - up) * 2 * q + up * (2 * (n - 1 - q) + 1)
    pos = (1 - core) * p + core * lax.rem(n - p, n)
    step = 1 - 2 * core
    follow = {"dp": 2 * chip_at(lax.rem(p + step + n, n)) + core}
    before = {"dp": 2 * chip_at(lax.rem(p - step + n, n)) + core}
    mate = {"dp": me + 1 - 2 * core}
    peer = {"tensor": 1 - side}

    def owner(r):
        return 2 * chip_at((1 - core) * r + core * lax.rem(n - r, n)) + core
    return me, side, core, pos, owner, follow, before, mate, peer


def forward_kernel(size, blk, count_ref, tok_ref, gain_ref, shift_ref, w_hbm, b_ref, up_hbm, down_hbm, mix_hbm,
                   ub_ref,
                   own_ref, oth_ref, qkv_ref, att_ref, recv_ref, lse_ref, upo_hbm, downo_hbm, mixo_hbm, ubo_ref,
                   acc_ref, top_ref, w_ref,
                   in_sem, a_send, a_recv, p_send, p_recv, us, ur, ums, umr, ds, dr, dms, dmr, t_send, t_recv):
    n = size // 2
    half, dim = tok_ref.shape
    width = w_ref.shape[1] // 3
    nb = 2 * half // blk
    me, side, core, pos, owner, follow, before, mate, peer = ring_place(size)
    w_copies = [pltpu.make_async_copy(w_hbm.at[j], w_ref.at[:, pl.ds(j * width, width)], in_sem.at[j])
                for j in range(3)]
    for copy in w_copies:
        copy.start()
    barrier = pltpu.get_barrier_semaphore()
    friends = [follow, before, mate, peer]
    for to in friends:
        pl.semaphore_signal(barrier, inc=1, device_id=to, device_id_type=pl.DeviceIdType.MESH)
    pl.semaphore_wait(barrier, len(friends))

    pieces = [remote(src.at[me], dst.at[me], p_send.at[k], p_recv.at[k], peer)
              for k, (src, dst) in enumerate(((up_hbm, upo_hbm), (down_hbm, downo_hbm)))]
    pieces += [remote(ub_ref, ubo_ref, p_send.at[2], p_recv.at[2], peer),
               remote(mix_hbm, mixo_hbm, p_send.at[3], p_recv.at[3], peer)]
    for piece in pieces[:3]:
        piece.start()

    def spread(ref, sems):
        return ring_spread(n, 1, pos, core, follow, mate,
                           lambda c, u: ref.at[owner(lax.rem(c - core * n - 1 + n, n))], *sems)
    rings = [spread(upo_hbm, (us, ur, ums, umr)), spread(downo_hbm, (ds, dr, dms, dmr))]

    def ticks(lo, hi):
        def one(k, _):
            @pl.when(k == 0)
            def _():
                pieces[0].wait_recv()
                pieces[1].wait_recv()
            for tick, _ in rings:
                tick(k, 0)
            return 0
        lax.fori_loop(lo, hi, one, 0)

    step = half // 4
    inner = step // 4

    def a_copy(i):
        at = pl.ds(pl.multiple_of(i * step, step), step)
        return remote(own_ref.at[at], oth_ref.at[at], a_send.at[i], a_recv.at[i], peer)

    def norm(i, _):
        def norm_rows(j, _):
            at = pl.ds(pl.multiple_of(i * step + j * inner, inner), inner)
            x = tok_ref[at, :].astype(f32)
            x = x - jnp.mean(x, axis=-1, keepdims=True)
            inv = lax.rsqrt(jnp.mean(x * x, axis=-1, keepdims=True) + EPSILON)
            own_ref[at, :] = (x * inv * gain_ref[...] + shift_ref[...]).astype(bf16)
            return 0
        lax.fori_loop(0, 4, norm_rows, 0)
        a_copy(i).start()
        return 0
    lax.fori_loop(0, 4, norm, 0)
    pieces[3].start()
    for copy in w_copies:
        copy.wait()

    def project(src, i, base):
        y = dot32(src[pl.ds(pl.multiple_of(i * step, step), step), :], w_ref[...])
        to = pl.ds(pl.multiple_of(base + i * step, step), step)
        for j in range(3):
            part = (y[:, j * width:(j + 1) * width] + b_ref[pl.ds(j, 1), :]).astype(bf16)
            qkv_ref[to, pl.ds(j * width, width)] = part * bf16(0.125) if j == 0 else part

    def own_project(i, _):
        project(own_ref, i, 0)
        return 0
    lax.fori_loop(0, 4, own_project, 0)

    def place(b):
        return pl.multiple_of(lax.rem(b + side * (nb // 2), nb) * blk, blk)
    lane_lo = lax.broadcasted_iota(jnp.int32, (blk, 128), 1) < HEAD
    count = count_ref[0]

    def block(qb, kb, masked):
        q_at, k_at = place(qb), place(kb)
        if masked:
            keep = (lax.broadcasted_iota(jnp.int32, (blk, blk), 1)
                    <= lax.broadcasted_iota(jnp.int32, (blk, blk), 0))
        else:
            apart = jnp.where(kb * count // nb == qb * count // nb, 0.0, -1e30)
        for pr in range(width // 128):
            q = qkv_ref[pl.ds(q_at, blk), pl.ds(128 * pr, 128)]
            k = qkv_ref[pl.ds(k_at, blk), pl.ds(width + 128 * pr, 128)]
            v = qkv_ref[pl.ds(k_at, blk), pl.ds(2 * width + 128 * pr, 128)]
            for h in range(2):
                mine = lane_lo if h == 0 else ~lane_lo
                head = 2 * pr + h
                s = dot_nt(jnp.where(mine, q, bf16(0)), k) * LOG2E
                s = jnp.where(keep, s, -1e30) if masked else s + apart
                top = jnp.max(s, axis=1, keepdims=True)
                vh = jnp.where(mine, v, bf16(1))
                if masked:
                    e = jnp.exp2(s - top)
                    acc_ref[qb, head] = dot32(e.astype(bf16), vh)
                    top_ref[qb, head] = jnp.broadcast_to(top, (blk, 128))
                else:
                    old = top_ref[qb, head]
                    new = jnp.maximum(old, top)
                    e = jnp.exp2(s - new[:, :1])
                    acc_ref[qb, head] = acc_ref[qb, head] * jnp.exp2(old - new) + dot32(e.astype(bf16), vh)
                    top_ref[qb, head] = new

    def t_copy(i):
        src = att_ref.at[pl.ds(pl.multiple_of(half + i * blk, blk), blk)]
        return remote(src, recv_ref.at[pl.ds(pl.multiple_of(i * blk, blk), blk)], t_send.at[i], t_recv.at[i], peer)

    def complete(qb):
        q_at = place(qb)
        for pr in range(width // 128):
            a0, a1 = acc_ref[qb, 2 * pr], acc_ref[qb, 2 * pr + 1]
            den = jnp.where(lane_lo, pltpu.roll(a0, HEAD, 1), pltpu.roll(a1, HEAD, 1))
            att_ref[pl.ds(q_at, blk), pl.ds(128 * pr, 128)] = (jnp.where(lane_lo, a0, a1) / den).astype(bf16)
            logs = (jnp.where(lane_lo, top_ref[qb, 2 * pr], top_ref[qb, 2 * pr + 1]) + jnp.log2(den)).T
            lse_ref[qb, pl.ds(2 * pr, 1), :] = logs[0:1]
            lse_ref[qb, pl.ds(2 * pr + 1, 1), :] = logs[HEAD:HEAD + 1]

        @pl.when(qb // (nb // 2) == 1 - side)
        def _():
            t_copy(lax.rem(qb, nb // 2)).start()

    def part(t, _):
        @pl.when(t == 1)
        def _():
            def other_project(i, _):
                ticks(n // 2 + i * (n - n // 2) // 4, n // 2 + (i + 1) * (n - n // 2) // 4)
                a_copy(i).wait_recv()
                project(oth_ref, i, half)
                return 0
            lax.fori_loop(0, 4, other_project, 0)

        @pl.when(t < 2)
        def _():
            base = (t + side - 2 * t * side) * (nb // 2)

            def queries(i, _):
                @pl.when(t == 0)
                def _():
                    ticks(i * n // nb, (i + 1) * n // nb)
                block(base + i, base + i, True)
                return 0
            lax.fori_loop(0, nb // 2, queries, 0)
        first = jnp.where(t < 2, (t + side - 2 * t * side) * (nb // 2), nb // 2)

        def rows_of(i, _):
            keys = jnp.where(t < 2, first, 0)
            stop = jnp.where(t < 2, i, nb // 2)

            def one(j, _):
                block(first + i, keys + j, False)
                return 0
            lax.fori_loop(0, stop, one, 0)

            @pl.when(t == 2)
            def _():
                complete(nb // 2 + i)
            return 0
        lax.fori_loop(0, nb // 2, rows_of, 0)

        @pl.when(t == 1)
        def _():
            def early(i, _):
                complete(i)
                return 0
            lax.fori_loop(0, nb // 2, early, 0)
        return 0
    lax.fori_loop(0, 3, part, 0)
    for i in range(4):
        a_copy(i).wait_send()
    for piece in pieces[:2]:
        piece.wait_send()
    for piece in pieces[2:]:
        piece.wait()
    for _, finish in rings:
        finish()
    for i in range(nb // 2):
        t_copy(i).wait()


def forward(size, count, tokens, gain, shift, w, bias, up, down, mix, up_bias, blk=512):
    half, dim = tokens.shape
    width = w.shape[2]
    hidden = up.shape[1]
    nb = 2 * half // blk
    n = size // 2
    heads = width // HEAD
    vm = pl.BlockSpec(memory_space=pltpu.VMEM)
    hb = pl.BlockSpec(memory_space=pl.ANY)
    sm = pl.BlockSpec(memory_space=pltpu.SMEM)
    V, S = pltpu.VMEM, pltpu.SemaphoreType.DMA
    up3, down3 = up.reshape(size, dim // size, hidden), down.reshape(size, hidden // size, dim)
    shape = jax.ShapeDtypeStruct
    outs = pl.pallas_call(
        functools.partial(forward_kernel, size, blk),
        in_specs=[sm, vm, vm, vm, hb, vm, hb, hb, hb, vm],
        out_specs=[vm] * 6 + [hb] * 3 + [vm],
        out_shape=[shape((half, dim), bf16), shape((half, dim), bf16), shape((2 * half, 3 * width), bf16),
                   shape((2 * half, width), bf16), shape((half, width), bf16), shape((nb, 8, blk), f32),
                   shape(up3.shape, bf16), shape(down3.shape, bf16), shape(mix.shape, bf16),
                   shape((2, dim), f32)],
        scratch_shapes=[V((nb, heads, blk, 128), f32), V((nb, heads, blk, 128), f32), V((dim, 3 * width), bf16),
                        S((3,)), S((4,)), S((4,)), S((4,)), S((4,)),
                        S((n - 1,)), S((n - 1,)), S((n,)), S((n,)), S((n - 1,)), S((n - 1,)), S((n,)), S((n,)),
                        S((nb // 2,)), S((nb // 2,))],
        compiler_params=pltpu.CompilerParams(collective_id=1, has_side_effects=True, vmem_limit_bytes=60 << 20),
        cost_estimate=pl.CostEstimate(flops=12_000_000_000, transcendentals=0, bytes_accessed=20_000_000),
        name="forward",
    )(count, tokens, gain[None], shift[None], w, bias, up3, down3, mix, up_bias.reshape(2, dim))
    a1, a1_other, qkv, att, recv, lse, upo, downo, mixo, ubo = outs
    return a1, a1_other, qkv, att, recv, lse, upo.reshape(dim, hidden), downo.reshape(hidden, dim), mixo, \
        ubo.reshape(hidden)


def mlp_kernel(a2_ref, gm_ref, mid_ref, up_ref, upo_ref, bias_ref, down_ref, downo_ref, dbias_ref,
               gd_ref, gu_ref, da2_ref, res_ref, small_ref,
               turn_ref, w_ref, v_ref, acc_ref):
    i = pl.program_id(0)
    steps = pl.num_programs(0)
    rows = a2_ref.shape[0]
    tile = w_ref.shape[1]

    @pl.when(i == 0)
    def _():
        turn_ref[...] = a2_ref[...].T
        da2_ref[...] = jnp.zeros_like(da2_ref)
        acc_ref[...] = jnp.zeros_like(acc_ref)
        small_ref[...] = jnp.zeros_like(small_ref)

    @pl.when(i < steps // 2)
    def _():
        w_ref[...] = up_ref[...]
        v_ref[...] = down_ref[...]

    @pl.when(i >= steps // 2)
    def _():
        w_ref[...] = upo_ref[...]
        v_ref[...] = downo_ref[...]
    half = rows // 2
    gd = gu = sums = None
    for r in range(2):
        at = pl.ds(r * half, half)
        gm = gm_ref[at, :]
        pre = dot32(a2_ref[at, :], w_ref[...]) + bias_ref[0]
        grad = dot_nt(gm, v_ref[...])
        act, slope = gelu_pair(pre)
        act = act.astype(bf16)
        grad = (grad * slope).astype(bf16)
        acc_ref[at, :] += dot32(act, v_ref[...])
        da2_ref[at, :] += dot_nt(grad, w_ref[...])
        gd1 = dot_tn(act, gm)
        gu1 = dot32(turn_ref[:, r * half:(r + 1) * half], grad)
        s1 = jnp.sum(grad.astype(f32), axis=0, keepdims=True)
        gd, gu, sums = (gd1, gu1, s1) if r == 0 else (gd + gd1, gu + gu1, sums + s1)
    gd_ref[0] = gd.astype(bf16)
    gu_ref[0] = gu.astype(bf16)
    small_ref[pl.ds(4 + i // 2, 1), pl.ds(pl.multiple_of(lax.rem(i, 2) * tile, 128), tile)] = sums

    @pl.when(i == steps - 1)
    def _():
        res_ref[...] = (mid_ref[...] + BRANCH * (acc_ref[...] + dbias_ref[...])).astype(bf16)


def mlp(a2, grad_mlp, middle, up, up_other, bias, bias_other, down, down_other, down_bias):
    rows, dim = a2.shape
    hidden = up.shape[1]
    tile = dim // 2
    per = hidden // tile
    bias = jnp.concatenate([bias, bias_other]).reshape(2 * per, 1, tile)
    whole = pl.BlockSpec((rows, dim), lambda i: (0, 0), pipeline_mode=pl.Buffered(1))
    first = lambda i: jnp.minimum(i, per - 1)
    later = lambda i: jnp.maximum(i - per, 0)
    return pl.pallas_call(
        mlp_kernel,
        grid=(2 * per,),
        in_specs=[whole, whole, whole,
                  pl.BlockSpec((dim, tile), lambda i: (0, first(i))),
                  pl.BlockSpec((dim, tile), lambda i: (0, later(i))),
                  pl.BlockSpec((1, 1, tile), lambda i: (i, 0, 0)),
                  pl.BlockSpec((tile, dim), lambda i: (first(i), 0)),
                  pl.BlockSpec((tile, dim), lambda i: (later(i), 0)),
                  pl.BlockSpec((1, dim), lambda i: (0, 0))],
        out_specs=[pl.BlockSpec((1, tile, dim), lambda i: (i // per, i % per, 0)),
                   pl.BlockSpec((1, dim, tile), lambda i: (i // per, i % per // 2, i % 2)),
                   pl.BlockSpec((rows, dim), lambda i: (0, 0)),
                   pl.BlockSpec((rows, dim), lambda i: (0, 0)),
                   pl.BlockSpec((8, dim), lambda i: (0, 0))],
        out_shape=[jax.ShapeDtypeStruct((2, hidden, dim), bf16),
                   jax.ShapeDtypeStruct((2, hidden, dim), bf16),
                   jax.ShapeDtypeStruct((rows, dim), f32),
                   jax.ShapeDtypeStruct((rows, dim), bf16),
                   jax.ShapeDtypeStruct((8, dim), f32)],
        scratch_shapes=[pltpu.VMEM((dim, rows), bf16), pltpu.VMEM((dim, tile), bf16), pltpu.VMEM((tile, dim), bf16),
                        pltpu.VMEM((rows, dim), f32)],
        compiler_params=pltpu.CompilerParams(vmem_limit_bytes=60 << 20),
        cost_estimate=pl.CostEstimate(flops=29_000_000_000, transcendentals=0, bytes_accessed=30_000_000),
        name="mlp",
    )(a2, grad_mlp, middle, up, up_other, bias, down, down_other, down_bias[None])


def row_stats(v):
    centre = jnp.mean(v, axis=-1, keepdims=True)
    centred = v - centre
    inv = lax.rsqrt(jnp.mean(centred * centred, axis=-1, keepdims=True) + EPSILON)
    return centre, inv


def dot32(a, b):
    return jnp.dot(a, b, preferred_element_type=f32)


def dot_nt(a, b):
    return lax.dot_general(a, b, NT, preferred_element_type=f32)


def dot_tn(a, b):
    return lax.dot_general(a, b, TN, preferred_element_type=f32)


def xor_step(v, size, bit):
    return lax.ppermute(v, "dp", [(i, i ^ (1 << bit)) for i in range(size)])


def gelu_pair(v):
    t = jnp.tanh(GELU_C * (v + 0.044715 * v * v * v))
    return 0.5 * v * (1.0 + t), 0.5 * (1.0 + t) + 0.5 * v * (1.0 - t * t) * (
        GELU_C * (1.0 + 3.0 * 0.044715 * v * v))


def local(
    tokens,
    seq_count,
    first_gain,
    first_shift,
    heads_weight,
    heads_bias,
    mixing_weight,
    mixing_bias,
    second_gain,
    second_shift,
    up_weight,
    up_bias,
    down_weight,
    down_bias,
    cotangent,
):
    size = lax.axis_size("dp")
    half, dim = tokens.shape
    width = heads_weight.shape[2]
    hidden = up_weight.shape[1]

    x = tokens.astype(f32)
    bias3 = jnp.stack([heads_bias[0], jnp.zeros_like(heads_bias[0]), heads_bias[1]])
    a1, a1_other, qkv, att, att_recv, lse, up_other, down_other, mix_other, up_bias_other = forward(
        size, seq_count, tokens, first_gain, first_shift, heads_weight, bias3, up_weight, down_weight, mixing_weight,
        up_bias)
    att_mine = att[:half]
    middle = x + BRANCH * (dot32(att_mine, mixing_weight) + dot32(att_recv, mix_other) + mixing_bias)
    centre2, inv2 = row_stats(middle)
    h2 = (middle - centre2) * inv2
    a2 = (h2 * second_gain + second_shift).astype(bf16)

    grad_mlp = (BRANCH * cotangent.astype(f32)).astype(bf16)
    gd, gu, grad_a2, result, small = mlp(a2, grad_mlp, middle, up_weight, up_other, up_bias, up_bias_other,
                                         down_weight, down_other, down_bias)
    fin, tail, grad_tokens, small, last = backward(
        size, seq_count, qkv, att, att_recv, lse, gd, gu, a1, a1_other, heads_weight, mixing_weight, mix_other, small,
        tokens, first_gain[None], second_gain[None], cotangent, middle, grad_a2)
    groups = 1.0 / size
    small = small * groups
    last = last * groups
    fin = fin.reshape(2, hidden, dim).astype(f32) * groups
    tail = tail.reshape(4 * dim, width).astype(f32) * groups
    grad_up = fin[1]
    return (
        result,
        grad_tokens,
        last[0],
        last[1],
        tail[:3 * dim].reshape(3, dim, width),
        last[2].reshape(2, width),
        jnp.concatenate([tail[3 * dim:3 * dim + width], tail[3 * dim + width:]], axis=1),
        small[3],
        small[1],
        small[2],
        jnp.concatenate([grad_up[:dim], grad_up[dim:]], axis=1),
        small[4:6].reshape(hidden),
        fin[0],
        small[0],
    )


def solution(mesh):
    placed = (
        P(("dp", "tensor"), None),
        P("dp"),
        P(),
        P(),
        P(None, None, "tensor"),
        P(None, "tensor"),
        P("tensor", None),
        P(),
        P(),
        P(),
        P(None, "tensor"),
        P("tensor"),
        P("tensor", None),
        P(),
        P(("dp", "tensor"), None),
    )
    return jax.shard_map(
        local,
        mesh=mesh,
        in_specs=placed,
        out_specs=(
            P(("dp", "tensor"), None),
            P(("dp", "tensor"), None),
            P(),
            P(),
            P(None, None, "tensor"),
            P(None, "tensor"),
            P("tensor", None),
            P(),
            P(),
            P(),
            P(None, "tensor"),
            P("tensor"),
            P("tensor", None),
            P(),
        ),
        check_vma=False,
    )
```
